512 devices in a mesh: rows: 64 (over x, y, z_hi, core), cols: 8 (over z_lo).
Axes of the slice: x: 4, y: 4, z: 16 (z_hi: 2, z_lo: 8; z = z_hi * 8 + z_lo), core: 2. Of those that a mesh axis runs over, the one named last changes fastest.
Arguments:
- homolog_embedding: bfloat16 [512, 1024, 256], P('rows', 'cols'), may hold values from -120 to 120
- couple_embedding: bfloat16 [1024, 1024, 128], P('rows', 'cols'), may hold values from -6 to 6
- homolog_standardize_factor: float32 [256], replicated, may hold values from 0.25 to 1.75
- first_factor_mapping: bfloat16 [256, 32], replicated, may hold values from -0.375 to 0.375
- second_factor_mapping: bfloat16 [256, 32], replicated, may hold values from -0.375 to 0.375
- contraction_to_couple_mapping: bfloat16 [1024, 128], replicated, may hold values from -4 to 4
- couple_standardize_factor: float32 [128], replicated, may hold values from 0.25 to 1.75
- widening_matrix: bfloat16 [128, 512], replicated, may hold values from -0.5 to 0.5
- narrowing_matrix: bfloat16 [512, 128], replicated, may hold values from -0.25 to 0.25
Outputs:
- pair_out: bfloat16 [1024, 1024, 128], P('rows', 'cols')
The draws below stay inside these ranges and needn't reach their ends.
All inputs are finite; a program needn't handle non-finite values.
Results may differ from the reference program's by a relative error of at most 0.0064.
Values may be sent and summed in bfloat16 or wider, within the bound.
A program may use at most 64 MiB of HBM per device.

```python
import math
import jax
import jax.numpy as jnp
from jax import lax

FEATURE_DEPTH = 256
FACTOR_DIM = 32
CZ = 128
FFN = 512
CHAIN_LENGTH = 1024
HOMOLOG_COUNT = 512


def draw_homolog_embedding(key, part):
    key_base = jax.random.fold_in(key, 11)
    key_rows = jax.random.fold_in(key, 12)
    random_seed_cols_draw = jax.random.fold_in(key, 13)
    complete_extent = (HOMOLOG_COUNT, CHAIN_LENGTH, FEATURE_DEPTH)
    row_scale = jnp.exp(jax.random.uniform(key_rows, (HOMOLOG_COUNT, CHAIN_LENGTH, 1), jnp.float32, 0.0, math.log(10.0)))
    per_feature_factor = jnp.exp(jax.random.uniform(random_seed_cols_draw, (1, 1, FEATURE_DEPTH), jnp.float32, math.log(0.5), math.log(2.0)))
    sampled_entries = jax.random.truncated_normal(key_base, -6.0, 6.0, complete_extent, jnp.float32)
    return (sampled_entries * per_feature_factor * row_scale).astype(jnp.bfloat16)


def shard_levels(stream_key, dims, split, least, top_value):
    factor_of = 1.0
    for dim, parts in split:
        draws = jax.random.uniform(jax.random.fold_in(jax.random.fold_in(stream_key, 6), dim), (parts,), jnp.float32, least / len(split), top_value / len(split))
        factor_of = factor_of * jnp.repeat(jnp.exp(draws), dims[dim] // parts).reshape((-1,) + (1,) * (len(dims) - 1 - dim))
    return factor_of


def noise(stream_key, extent, width, reach, shards=(), dtype=jnp.bfloat16):
    drawn = jax.random.normal(stream_key, extent, jnp.float32) * width
    if len(shards) > 0:
        drawn = shard_levels(stream_key, extent, shards, -0.22, 0.18) * drawn
    return jnp.clip(drawn, min=-reach, max=reach).astype(dtype)


def setup_inputs(seed: int = 0) -> dict:
    key_list = jax.random.split(jax.random.key(seed), 10)
    return {
        "homolog_embedding": draw_homolog_embedding(jax.random.fold_in(key_list[9], 71), 0),
        "couple_embedding": noise(key_list[1], (CHAIN_LENGTH, CHAIN_LENGTH, CZ), 1.0, 6.0, ((0, 64), (1, 8))),
        "homolog_standardize_factor": jnp.clip(1.0 + 0.15 * jax.random.normal(key_list[2], (FEATURE_DEPTH,), jnp.float32), 0.25, 1.75),
        "first_factor_mapping": noise(key_list[3], (FEATURE_DEPTH, FACTOR_DIM), FEATURE_DEPTH ** -0.5, 0.375),
        "second_factor_mapping": noise(key_list[4], (FEATURE_DEPTH, FACTOR_DIM), FEATURE_DEPTH ** -0.5, 0.375),
        "contraction_to_couple_mapping": noise(key_list[5], (FACTOR_DIM * FACTOR_DIM, CZ), (max(1, FACTOR_DIM * FACTOR_DIM // HOMOLOG_COUNT)) ** -0.5, 4.0),
        "couple_standardize_factor": jnp.clip(1.0 + 0.15 * jax.random.normal(key_list[6], (CZ,), jnp.float32), 0.25, 1.75),
        "widening_matrix": noise(key_list[7], (CZ, FFN), CZ ** -0.5, 0.5),
        "narrowing_matrix": noise(key_list[8], (FFN, CZ), FFN ** -0.5, 0.25),
    }


def standardize_features(sampled_entries, gain_vector):
    floats = sampled_entries.astype(jnp.float32)
    average = lax.optimization_barrier(jnp.mean(floats, axis=-1, keepdims=True))
    centred = floats - average
    variance = lax.optimization_barrier(jnp.mean(centred * centred, axis=-1, keepdims=True))
    return centred * lax.rsqrt(variance + 1e-05) * gain_vector.astype(jnp.float32)

def reference(homolog_embedding, couple_embedding, homolog_standardize_factor, first_factor_mapping, second_factor_mapping, contraction_to_couple_mapping, couple_standardize_factor, widening_matrix, narrowing_matrix):
    standardized_tensor = standardize_features(homolog_embedding, homolog_standardize_factor).astype(jnp.bfloat16)
    unrolled_tensor = standardized_tensor.reshape(HOMOLOG_COUNT * CHAIN_LENGTH, FEATURE_DEPTH)
    left_rows = jnp.dot(unrolled_tensor, first_factor_mapping, preferred_element_type=jnp.float32).astype(jnp.bfloat16).reshape(HOMOLOG_COUNT, CHAIN_LENGTH, FACTOR_DIM)
    right_rows = jnp.dot(unrolled_tensor, second_factor_mapping, preferred_element_type=jnp.float32).astype(jnp.bfloat16).reshape(HOMOLOG_COUNT, CHAIN_LENGTH, FACTOR_DIM)
    block = math.gcd(CHAIN_LENGTH, 16)
    block_count = CHAIN_LENGTH // block
    left_blocks = left_rows.reshape(HOMOLOG_COUNT, block_count, block, FACTOR_DIM).transpose(1, 0, 2, 3)
    right_float = right_rows.astype(jnp.float32)

    def project_block(left_block):
        outer_product = jnp.einsum('sip,sjq->ijpq', left_block.astype(jnp.float32), right_float) / HOMOLOG_COUNT
        outer_product = outer_product.astype(jnp.bfloat16).reshape(block * CHAIN_LENGTH, FACTOR_DIM * FACTOR_DIM)
        return jnp.dot(outer_product, contraction_to_couple_mapping, preferred_element_type=jnp.float32).reshape(block, CHAIN_LENGTH, CZ)
    update = lax.map(project_block, left_blocks).reshape(CHAIN_LENGTH, CHAIN_LENGTH, CZ)
    pair_mid = couple_embedding.astype(jnp.float32) + update
    pair_normed = standardize_features(pair_mid, couple_standardize_factor).astype(jnp.bfloat16).reshape(CHAIN_LENGTH * CHAIN_LENGTH, CZ)
    hidden = jnp.maximum(jnp.dot(pair_normed, widening_matrix, preferred_element_type=jnp.float32), 0.0).astype(jnp.bfloat16)
    result = pair_mid + jnp.dot(hidden, narrowing_matrix, preferred_element_type=jnp.float32).reshape(CHAIN_LENGTH, CHAIN_LENGTH, CZ)
    return result.astype(jnp.bfloat16)
```

```python
import jax
import jax.numpy as jnp
from jax import lax
from jax.experimental import pallas as pl
from jax.experimental.pallas import tpu as pltpu
from jax.sharding import PartitionSpec as P

MESH = pl.DeviceIdType.MESH
F32 = jnp.float32
BF16 = jnp.bfloat16
EPS = 1e-5


def kernel(
    x_ref,
    cpl_hbm,
    g1_ref,
    w1_ref,
    w2_ref,
    w3_hbm,
    g2_ref,
    wa_hbm,
    wb_hbm,
    out_ref,
    cpl_ref,
    w3_ref,
    wa_ref,
    wb_ref,
    w3f_ref,
    wt_ref,
    xn_ref,
    tf_ref,
    lx_ref,
    rx_ref,
    xl_ref,
    xr_ref,
    lloc_ref,
    lz_ref,
    lb_ref,
    lt_ref,
    rb_ref,
    oall_ref,
    in_sem,
    xsend,
    xrecv,
    rsend,
    rrecv,
    sibsend,
    sibrecv,
    zsend,
    zrecv,
    psend,
    precv,
):
    r = lax.axis_index("rows")
    zl = lax.axis_index("cols")
    core = r % 2
    zh = (r // 2) % 2
    y = (r // 4) % 4
    x = r // 16
    z = zh * 8 + zl

    def rows_of(xx, yy, hh, kk):
        return ((xx * 4 + yy) * 2 + hh) * 2 + kk

    sib = (rows_of(x, y, zh, 1 - core), zl)

    def plane(d):
        px = (x + d // 4) % 4
        py = (y + d % 4) % 4
        return px, py

    def zdev(dz):
        zz = (z + dz) % 16
        return (rows_of(x, y, zz // 8, core), zz % 8)

    barrier = pltpu.get_barrier_semaphore()
    pl.semaphore_signal(barrier, inc=1, device_id=sib, device_id_type=MESH)

    def greet_plane(d, _):
        px, py = plane(d)
        pl.semaphore_signal(
            barrier, inc=1, device_id=(rows_of(px, py, zh, core), zl), device_id_type=MESH
        )
        return 0

    lax.fori_loop(1, 16, greet_plane, 0)

    def greet_z(d, _):
        pl.semaphore_signal(barrier, inc=1, device_id=zdev(d), device_id_type=MESH)
        return 0

    lax.fori_loop(1, 16, greet_z, 0)

    loads = [
        pltpu.make_async_copy(src, dst, in_sem.at[n])
        for n, (src, dst) in enumerate(
            [(w3_hbm, w3_ref), (cpl_hbm, cpl_ref), (wa_hbm, wa_ref), (wb_hbm, wb_ref)]
        )
    ]
    for load in loads:
        load.start()

    gain = g1_ref[...]
    for s in range(8):
        xs = x_ref[s].astype(F32)
        mean = jnp.mean(xs, axis=-1, keepdims=True)
        cen = xs - mean
        var = jnp.mean(cen * cen, axis=-1, keepdims=True)
        xn_ref[s * 128 : (s + 1) * 128, :] = (cen * lax.rsqrt(var + EPS) * gain).astype(BF16)
    w1 = w1_ref[...]
    w2 = w2_ref[...]
    wcat = jnp.concatenate([w1] * 4 + [w2] * 4, axis=1)
    for s in range(8):
        both = jnp.dot(xn_ref[s * 128 : (s + 1) * 128, :], wcat, preferred_element_type=F32)
        tf_ref[pl.ds(s, 128, stride=8), :] = both[:, :128]
        right = both[:, 128:].T
        rx_ref[pl.ds(s, 32, stride=8), :] = right[:32]
    lane = lax.broadcasted_iota(jnp.int32, (8, 128), 1) // 32
    for kk in range(2):
        for hh in range(2):
            for yy in range(2):
                gg = yy * 4 + hh * 2 + kk
                for g in range(4):
                    base = (gg * 16 + g * 4) * 8
                    tile = tf_ref[base : base + 8, :]
                    for e in range(1, 4):
                        other = tf_ref[base + e * 8 : base + e * 8 + 8, :]
                        tile = jnp.where(lane == e, other, tile)
                    lx_ref[kk, hh * 2 + yy, :, g * 128 : (g + 1) * 128] = tile

    pl.semaphore_wait(barrier, 31)

    def swap(n):
        if n == 0:
            src, dst = rx_ref.at[pl.ds(pl.multiple_of((1 - core) * 128, 128), 128)], xr_ref.at[core]
        else:
            src, dst = lx_ref.at[1 - core], xl_ref.at[core]
        return pltpu.make_async_remote_copy(
            src_ref=src,
            dst_ref=dst,
            send_sem=xsend.at[n],
            recv_sem=xrecv.at[n],
            device_id=sib,
            device_id_type=MESH,
        )

    def swap_in(n):
        dst = xr_ref.at[1 - core] if n == 0 else xl_ref.at[1 - core]
        return pltpu.make_async_remote_copy(
            src_ref=dst,
            dst_ref=dst,
            send_sem=xsend.at[n],
            recv_sem=xrecv.at[n],
            device_id=sib,
            device_id_type=MESH,
        )

    swap(0).start()
    swap(1).start()
    xr_ref[core] = rx_ref[pl.ds(pl.multiple_of(core * 128, 128), 128), :]
    xl_ref[core] = lx_ref[core]
    mine = zh * 16 + x * 4 + y
    swap_in(0).wait_recv()
    for q in range(16):
        rb_ref[core, mine, :, q * 128 : (q + 1) * 128] = jnp.concatenate(
            [xr_ref[0, q * 8 : (q + 1) * 8, :], xr_ref[1, q * 8 : (q + 1) * 8, :]], axis=0
        ).astype(BF16)

    def rcopy(slot, dev, sem):
        return pltpu.make_async_remote_copy(
            src_ref=rb_ref.at[core, slot],
            dst_ref=rb_ref.at[core, slot],
            send_sem=rsend.at[sem],
            recv_sem=rrecv.at[slot],
            device_id=dev,
            device_id_type=MESH,
        )

    def scopy(slot, half):
        return pltpu.make_async_remote_copy(
            src_ref=rb_ref.at[half, slot],
            dst_ref=rb_ref.at[half, slot],
            send_sem=sibsend.at[slot],
            recv_sem=sibrecv.at[slot],
            device_id=sib,
            device_id_type=MESH,
        )

    partner = (1 - zh) * 16 + x * 4 + y
    zpart = (rows_of(x, y, 1 - zh, core), zl)

    def adev(e):
        return (rows_of((x + e * (1 - core)) % 4, (y + e * core) % 4, zh, core), zl)

    def bdev(e):
        return (rows_of((x + e * core) % 4, (y + e * (1 - core)) % 4, zh, core), zl)

    def aslot(e, hh):
        return hh * 16 + ((x + (4 - e) * (1 - core)) % 4) * 4 + (y + (4 - e) * core) % 4

    def send_a(hh, base):
        def body(e, _):
            rcopy(aslot(0, hh), adev(e), base + e - 1).start()
            return 0

        lax.fori_loop(1, 4, body, 0)

    def send_b(hh, base, a):
        def body(e, _):
            rcopy(aslot(a, hh), bdev(e), base + a * 3 + e - 1).start()
            return 0

        lax.fori_loop(1, 4, body, 0)

    rcopy(mine, zpart, 0).start()
    send_a(zh, 1)
    send_b(zh, 7, 0)

    swap_in(1).wait_recv()
    for hy in range(4):
        for g in range(4):
            cols = slice(g * 128, (g + 1) * 128)
            lloc_ref[hy // 2, hy % 2, :, cols] = jnp.concatenate(
                [xl_ref[0, hy, :, cols], xl_ref[1, hy, :, cols]], axis=0
            ).astype(BF16)

    def zcopy(dz):
        zz = (z + dz) % 16
        return pltpu.make_async_remote_copy(
            src_ref=lloc_ref.at[zz // 8],
            dst_ref=lz_ref.at[z],
            send_sem=zsend.at[dz],
            recv_sem=zrecv.at[z],
            device_id=zdev(dz),
            device_id_type=MESH,
        )

    def zcopy_in(zz):
        return pltpu.make_async_remote_copy(
            src_ref=lz_ref.at[zz],
            dst_ref=lz_ref.at[zz],
            send_sem=zsend.at[0],
            recv_sem=zrecv.at[zz],
            device_id=zdev(1),
            device_id_type=MESH,
        )

    def zstart(n, _):
        dz = (8 + ((n + 1) // 2) * (1 - 2 * (n % 2)) + 16) % 16
        zcopy(dz).start()
        return 0

    lax.fori_loop(0, 15, zstart, 0)
    lz_ref[z] = lloc_ref[zh]
    scopy(mine, core).start()

    def fwd_a(hh, base):
        def body(e, _):
            slot = aslot(e, hh)
            rcopy(slot, adev(1), 0).wait_recv()
            send_b(hh, base, e)
            scopy(slot, core).start()
            return 0

        lax.fori_loop(1, 4, body, 0)

    fwd_a(zh, 7)

    loads[0].wait()
    for p in range(32):
        w3f_ref[pl.ds(p, 32, stride=32), :] = w3_ref[p * 32 : (p + 1) * 32, :].astype(F32)
    for n in range(8):
        wt_ref[:, n * 128 : (n + 1) * 128] = w3f_ref[n * 128 : (n + 1) * 128, :].T.astype(BF16)

    rcopy(partner, zpart, 0).wait_recv()
    send_a(1 - zh, 4)
    send_b(1 - zh, 19, 0)
    scopy(partner, core).start()
    fwd_a(1 - zh, 19)

    def pcopy(d, hh):
        px, py = plane(d)
        return pltpu.make_async_remote_copy(
            src_ref=lz_ref.at[hh * 8 + px * 2 + py // 2, py % 2],
            dst_ref=lb_ref.at[hh * 16 + x * 4 + y],
            send_sem=psend.at[d * 2 + hh],
            recv_sem=precv.at[hh * 16 + x * 4 + y],
            device_id=(rows_of(px, py, zh, core), zl),
            device_id_type=MESH,
        )

    def pcopy_in(slot):
        return pltpu.make_async_remote_copy(
            src_ref=lb_ref.at[slot],
            dst_ref=lb_ref.at[slot],
            send_sem=psend.at[0],
            recv_sem=precv.at[slot],
            device_id=sib,
            device_id_type=MESH,
        )

    def zwait(dz, _):
        zcopy_in((z + dz) % 16).wait_recv()
        return 0

    lax.fori_loop(1, 16, zwait, 0)

    def pstart(d, _):
        for hh in range(2):
            pcopy(d, hh).start()
        return 0

    lax.fori_loop(1, 16, pstart, 0)
    for hh in range(2):
        lb_ref[hh * 16 + x * 4 + y] = lz_ref[hh * 8 + x * 2 + y // 2, y % 2]

    def bslot(n, hh):
        e = n // 4 + 1
        a = n % 4
        return (
            hh * 16
            + ((x + (4 - a) * (1 - core) + (4 - e) * core) % 4) * 4
            + (y + (4 - a) * core + (4 - e) * (1 - core)) % 4
        )

    def fwd_sib(hh):
        def body(n, _):
            slot = bslot(n, hh)
            rcopy(slot, adev(1), 0).wait_recv()
            scopy(slot, core).start()
            return 0

        lax.fori_loop(0, 12, body, 0)

    fwd_sib(zh)
    fwd_sib(1 - zh)

    def pwait(d, _):
        px, py = plane(d)
        for hh in range(2):
            pcopy_in(hh * 16 + px * 4 + py).wait_recv()
        return 0

    lax.fori_loop(1, 16, pwait, 0)
    for n in range(4):
        for m in range(4):
            lt_ref[m * 128 : (m + 1) * 128, n * 128 : (n + 1) * 128] = (
                lb_ref[n * 8 : (n + 1) * 8, :, m * 128 : (m + 1) * 128].reshape(128, 128).T
            )

    def sibwait(slot, _):
        scopy(slot, 1 - core).wait_recv()
        return 0

    lax.fori_loop(0, 32, sibwait, 0)

    for h in range(2):

        def outer(qb, _, h=h):
            off = pl.multiple_of(qb * 256, 256)
            right = rb_ref[h, :, :, pl.ds(off, 256)].reshape(512, 256)
            prod = jnp.dot(lt_ref[...], right, preferred_element_type=F32).astype(BF16)
            row = pl.multiple_of((h * 16 + qb * 2) * 32, 64)
            for i in range(16):
                for q in range(2):
                    oall_ref[
                        i // 2, pl.ds(row + q * 32, 32), (i % 2) * 128 : (i % 2 + 1) * 128
                    ] = prod[i * 32 : (i + 1) * 32, q * 128 : (q + 1) * 128]
            return 0

        lax.fori_loop(0, 8, outer, 0)

    for load in loads[1:]:
        load.wait()
    gain2 = g2_ref[...]

    def finish(n, _):
        for m in range(2):
            up = jnp.dot(wt_ref[...], oall_ref[n * 2 + m], preferred_element_type=F32)
            mids = []
            for k in range(2):
                i = n * 4 + m * 2 + k
                mids.append(
                    cpl_ref[i].astype(F32) + up[:, k * 128 : (k + 1) * 128].T * (1.0 / 512.0)
                )
            mid = jnp.concatenate(mids, axis=0)
            mean = jnp.mean(mid, axis=-1, keepdims=True)
            cen = mid - mean
            var = jnp.mean(cen * cen, axis=-1, keepdims=True)
            normed = (cen * lax.rsqrt(var + EPS) * gain2).astype(BF16)
            hidden = jnp.maximum(
                jnp.dot(normed, wa_ref[...], preferred_element_type=F32), 0.0
            ).astype(BF16)
            res = mid + jnp.dot(hidden, wb_ref[...], preferred_element_type=F32)
            out_ref[pl.ds(n * 4 + m * 2, 2)] = res.astype(BF16).reshape(2, 128, 128)
        return 0

    lax.fori_loop(0, 4, finish, 0)

    swap(0).wait_send()
    swap(1).wait_send()

    def rsent(n, _):
        rcopy(mine, zpart, n).wait_send()
        return 0

    lax.fori_loop(0, 31, rsent, 0)

    def sibsent(n, _):
        scopy(n, core).wait_send()
        return 0

    lax.fori_loop(0, 32, sibsent, 0)

    def zsent(n, _):
        zcopy(n).wait_send()
        return 0

    lax.fori_loop(1, 16, zsent, 0)

    def psent(n, _):
        for hh in range(2):
            pcopy(n, hh).wait_send()
        return 0

    lax.fori_loop(1, 16, psent, 0)


def on_device(x, cpl, g1, w1, w2, w3, g2, wa, wb):
    vmem = pl.BlockSpec(memory_space=pltpu.VMEM)
    hbm = pl.BlockSpec(memory_space=pl.ANY)
    dma = pltpu.SemaphoreType.DMA
    return pl.pallas_call(
        kernel,
        out_shape=jax.ShapeDtypeStruct(cpl.shape, BF16),
        in_specs=[vmem, hbm, vmem, vmem, vmem, hbm, vmem, hbm, hbm],
        out_specs=vmem,
        scratch_shapes=[
            pltpu.VMEM((16, 128, 128), BF16),
            pltpu.VMEM((1024, 128), BF16),
            pltpu.VMEM((128, 512), BF16),
            pltpu.VMEM((512, 128), BF16),
            pltpu.VMEM((1024, 128), F32),
            pltpu.VMEM((128, 1024), BF16),
            pltpu.VMEM((1024, 256), BF16),
            pltpu.VMEM((1024, 128), F32),
            pltpu.VMEM((2, 4, 8, 512), F32),
            pltpu.VMEM((256, 128), F32),
            pltpu.VMEM((2, 4, 8, 512), F32),
            pltpu.VMEM((2, 128, 128), F32),
            pltpu.VMEM((2, 2, 16, 512), BF16),
            pltpu.VMEM((16, 2, 16, 512), BF16),
            pltpu.VMEM((32, 16, 512), BF16),
            pltpu.VMEM((512, 512), BF16),
            pltpu.VMEM((2, 32, 16, 2048), BF16),
            pltpu.VMEM((8, 1024, 256), BF16),
            dma((4,)),
            dma((2,)),
            dma((2,)),
            dma((31,)),
            dma((32,)),
            dma((32,)),
            dma((32,)),
            dma((16,)),
            dma((16,)),
            dma((32,)),
            dma((32,)),
        ],
        compiler_params=pltpu.CompilerParams(
            collective_id=0, has_side_effects=True, vmem_limit_bytes=48 * 1024 * 1024
        ),
    )(x, cpl, g1.reshape(1, 256), w1, w2, w3, g2.reshape(1, 128), wa, wb)


def solution(mesh):
    return jax.shard_map(
        on_device,
        mesh=mesh,
        in_specs=(
            P("rows", "cols", None),
            P("rows", "cols", None),
            P(),
            P(),
            P(),
            P(),
            P(),
            P(),
            P(),
        ),
        out_specs=P("rows", "cols", None),
        check_vma=False,
    )
```

```python
import jax
import jax.numpy as jnp
from jax import lax
from jax.experimental import pallas as pl
from jax.experimental.pallas import tpu as pltpu
from jax.sharding import PartitionSpec as P

MESH = pl.DeviceIdType.MESH
F32 = jnp.float32
BF16 = jnp.bfloat16
EPS = 1e-5


def kernel(
    x_hbm,
    cpl_hbm,
    g1_hbm,
    w1_hbm,
    w2_hbm,
    w3_hbm,
    g2_hbm,
    wa_hbm,
    wb_hbm,
    out_ref,
    x_ref,
    cpl_ref,
    g1_ref,
    w1_ref,
    w2_ref,
    w3_ref,
    g2_ref,
    wa_ref,
    wb_ref,
    w3f_ref,
    wt_ref,
    xn_ref,
    tf_ref,
    lx_ref,
    rx_ref,
    xl_ref,
    xr_ref,
    lz_ref,
    lb_ref,
    lt_ref,
    rb_ref,
    oall_ref,
    in_sem,
    xsend,
    xrecv,
    rsend,
    rrecv,
    sibsend,
    sibrecv,
    zsend,
    zrecv,
    psend,
    precv,
):
    r = lax.axis_index("rows")
    zl = lax.axis_index("cols")
    core = r % 2
    zh = (r // 2) % 2
    y = (r // 4) % 4
    x = r // 16
    z = zh * 8 + zl

    loads = [
        pltpu.make_async_copy(src, dst, in_sem.at[n])
        for n, (src, dst) in enumerate(
            [
                (x_hbm, x_ref),
                (g1_hbm, g1_ref),
                (w1_hbm, w1_ref),
                (w2_hbm, w2_ref),
                (w3_hbm, w3_ref),
                (cpl_hbm, cpl_ref),
                (g2_hbm, g2_ref),
                (wa_hbm, wa_ref),
                (wb_hbm, wb_ref),
            ]
        )
    ]
    for load in loads:
        load.start()

    def rows_of(xx, yy, hh, kk):
        return ((xx * 4 + yy) * 2 + hh) * 2 + kk

    sib = (rows_of(x, y, zh, 1 - core), zl)

    def zdev(dz):
        zz = (z + dz + 16) % 16
        return (rows_of(x, y, zz // 8, core), zz % 8)

    barrier = pltpu.get_barrier_semaphore()
    pl.semaphore_signal(barrier, inc=1, device_id=sib, device_id_type=MESH)
    for dz in (8, 1, -1):
        pl.semaphore_signal(barrier, inc=1, device_id=zdev(dz), device_id_type=MESH)

    def greet_plane(d, _):
        px = (x + d // 4) % 4
        py = (y + d % 4) % 4
        pl.semaphore_signal(
            barrier, inc=1, device_id=(rows_of(px, py, zh, core), zl), device_id_type=MESH
        )
        return 0

    lax.fori_loop(1, 16, greet_plane, 0)

    for load in loads[:4]:
        load.wait()
    gain = g1_ref[...]
    for s in range(8):
        xs = x_ref[s].astype(F32)
        mean = jnp.mean(xs, axis=-1, keepdims=True)
        cen = xs - mean
        var = jnp.mean(cen * cen, axis=-1, keepdims=True)
        xn_ref[s * 128 : (s + 1) * 128, :] = (cen * lax.rsqrt(var + EPS) * gain).astype(BF16)
    wcat = jnp.concatenate([w1_ref[...]] * 4 + [w2_ref[...]] * 4, axis=0)
    for s in range(8):
        both = lax.dot_general(
            xn_ref[s * 128 : (s + 1) * 128, :],
            wcat,
            (((1,), (1,)), ((), ())),
            preferred_element_type=F32,
        )
        tf_ref[pl.ds(s, 128, stride=8), :] = both[:, :128]
        right = both[:, 128:].T
        rx_ref[pl.ds(s, 32, stride=8), :] = right[:32]
    lane = lax.broadcasted_iota(jnp.int32, (8, 128), 1) // 32
    for kk in range(2):
        for hh in range(2):
            for yy in range(2):
                gg = yy * 4 + hh * 2 + kk
                for g in range(4):
                    base = (gg * 16 + g * 4) * 8
                    tile = tf_ref[base : base + 8, :]
                    for e in range(1, 4):
                        other = tf_ref[base + e * 8 : base + e * 8 + 8, :]
                        tile = jnp.where(lane == e, other, tile)
                    lx_ref[kk, hh * 2 + yy, :, g * 128 : (g + 1) * 128] = tile

    loads[4].wait()
    for p in range(32):
        w3f_ref[pl.ds(p, 32, stride=32), :] = w3_ref[p * 32 : (p + 1) * 32, :].astype(F32)
    for n in range(8):
        wt_ref[:, n * 128 : (n + 1) * 128] = w3f_ref[n * 128 : (n + 1) * 128, :].T.astype(BF16)

    pl.semaphore_wait(barrier, 19)

    def swap(n):
        if n == 0:
            src, dst = rx_ref.at[pl.ds(pl.multiple_of((1 - core) * 128, 128), 128)], xr_ref.at[core]
        else:
            src, dst = lx_ref.at[1 - core], xl_ref.at[core]
        return pltpu.make_async_remote_copy(
            src_ref=src,
            dst_ref=dst,
            send_sem=xsend.at[n],
            recv_sem=xrecv.at[n],
            device_id=sib,
            device_id_type=MESH,
        )

    def swap_in(n):
        dst = xr_ref.at[1 - core] if n == 0 else xl_ref.at[1 - core]
        return pltpu.make_async_remote_copy(
            src_ref=dst,
            dst_ref=dst,
            send_sem=xsend.at[n],
            recv_sem=xrecv.at[n],
            device_id=sib,
            device_id_type=MESH,
        )

    swap(1).start()
    swap(0).start()
    xr_ref[core] = rx_ref[pl.ds(pl.multiple_of(core * 128, 128), 128), :]
    xl_ref[core] = lx_ref[core]

    def zcopy(up, origin, part, sem):
        return pltpu.make_async_remote_copy(
            src_ref=lz_ref.at[origin, part],
            dst_ref=lz_ref.at[origin, part],
            send_sem=zsend.at[up, sem, part],
            recv_sem=zrecv.at[origin, part],
            device_id=zdev(1 if up == 0 else -1),
            device_id_type=MESH,
        )

    def chain(up, d):
        if up == 0:
            nxt = (z + 1) % 16
            return (z - d + 16) % 16, nxt // 8, d < nxt % 8
        nxt = (z + 15) % 16
        return (z + d) % 16, nxt // 8, d < 6 - nxt % 8

    def zforward(up, d, act):
        origin, part, both = chain(up, d)
        act(zcopy(up, origin, part, d))

        @pl.when(both)
        def _():
            act(zcopy(up, origin, 1 - part, d))

    def zarrive(up, d):
        origin = chain(up, d)[0]
        zcopy(up, origin, zh, 0).wait_recv()
        other = (d - 1 < zl) if up == 0 else (d - 1 < 6 - zl)

        @pl.when(other)
        def _():
            zcopy(up, origin, 1 - zh, 0).wait_recv()

    def pcopy(origin, py2):
        cc = origin % 8
        return pltpu.make_async_remote_copy(
            src_ref=lz_ref.at[origin, zh, py2],
            dst_ref=lb_ref.at[(origin // 8) * 16 + x * 4 + y],
            send_sem=psend.at[0],
            recv_sem=precv.at[(origin // 8) * 16 + x * 4 + y],
            device_id=(rows_of(cc // 2, (cc % 2) * 2 + py2, zh, core), zl),
            device_id_type=MESH,
        )

    def spread(origin):
        cc = origin % 8

        def body(py2, _):
            here = jnp.logical_and(cc // 2 == x, (cc % 2) * 2 + py2 == y)

            @pl.when(here)
            def _():
                lb_ref[(origin // 8) * 16 + x * 4 + y] = lz_ref[origin, zh, py2]

            @pl.when(jnp.logical_not(here))
            def _():
                pcopy(origin, py2).start()

            return 0

        lax.fori_loop(0, 2, body, 0)

    def start(copy):
        copy.start()

    def sent(copy):
        copy.wait_send()

    swap_in(1).wait_recv()
    for hy in range(4):
        for g in range(4):
            cols = slice(g * 128, (g + 1) * 128)
            lz_ref[z, hy // 2, hy % 2, :, cols] = jnp.concatenate(
                [xl_ref[0, hy, :, cols], xl_ref[1, hy, :, cols]], axis=0
            ).astype(BF16)
    zforward(0, 0, start)
    zforward(1, 0, start)

    mine = zh * 16 + x * 4 + y
    swap_in(0).wait_recv()
    for q in range(16):
        rb_ref[core, mine, :, q * 128 : (q + 1) * 128] = jnp.concatenate(
            [xr_ref[0, q * 8 : (q + 1) * 8, :], xr_ref[1, q * 8 : (q + 1) * 8, :]], axis=0
        ).astype(BF16)

    def at(da, db):
        px = (x + da * (1 - core) + db * core + 4) % 4
        py = (y + da * core + db * (1 - core) + 4) % 4
        return px, py

    def slot_of(da, db, hh):
        px, py = at(da, db)
        return hh * 16 + px * 4 + py

    def dev_of(da, db):
        px, py = at(da, db)
        return (rows_of(px, py, zh, core), zl)

    zpart = zdev(8)

    def rfull(slot, dev):
        return pltpu.make_async_remote_copy(
            src_ref=rb_ref.at[core, slot],
            dst_ref=rb_ref.at[core, slot],
            send_sem=rsend.at[0],
            recv_sem=rrecv.at[slot, 0],
            device_id=dev,
            device_id_type=MESH,
        )

    def rhalf(slot, part, dev):
        piece = rb_ref.at[core, slot, :, pl.ds(part * 1024, 1024)]
        return pltpu.make_async_remote_copy(
            src_ref=piece,
            dst_ref=piece,
            send_sem=rsend.at[0],
            recv_sem=rrecv.at[slot, part],
            device_id=dev,
            device_id_type=MESH,
        )

    def scopy(slot):
        return pltpu.make_async_remote_copy(
            src_ref=rb_ref.at[core, slot],
            dst_ref=rb_ref.at[core, slot],
            send_sem=sibsend.at[0],
            recv_sem=sibrecv.at[0],
            device_id=sib,
            device_id_type=MESH,
        )

    steps = (0, -1, 1, 2)

    def begin(hh):
        slot = slot_of(0, 0, hh)
        for da, db in ((1, 0), (-1, 0), (0, 1), (0, -1)):
            rfull(slot, dev_of(da, db)).start()
        scopy(slot).start()

    def to_b(slot):
        rfull(slot, dev_of(0, 1)).start()
        rfull(slot, dev_of(0, -1)).start()
        scopy(slot).start()

    def ring_a(hh):
        for part in range(2):
            step = 1 - 2 * part
            slot = slot_of(-step, 0, hh)
            rfull(slot, dev_of(step, 0)).wait_recv()
            rhalf(slot, part, dev_of(step, 0)).start()
            to_b(slot)

    def ring_a_far(hh):
        slot = slot_of(2, 0, hh)
        for part in range(2):
            rhalf(slot, part, dev_of(1, 0)).wait_recv()
        to_b(slot)

    def ring_b(hh, n):
        for part in range(2):
            step = 1 - 2 * part
            slot = slot_of(steps[n], -step, hh)
            rfull(slot, dev_of(0, step)).wait_recv()
            rhalf(slot, part, dev_of(0, step)).start()
            scopy(slot).start()

    def ring_b_far(hh, n):
        slot = slot_of(steps[n], 2, hh)
        for part in range(2):
            rhalf(slot, part, dev_of(0, 1)).wait_recv()
        scopy(slot).start()

    begin(zh)
    rfull(mine, zpart).start()
    spread(z)

    def zstep(d):
        zarrive(0, d)
        if d < 8:
            zforward(0, d, start)
            zarrive(1, d)
            if d < 7:
                zforward(1, d, start)
        spread(chain(0, d)[0])
        if d < 8:
            spread(chain(1, d)[0])

    other = 1 - zh
    zstep(1)
    ring_a(zh)
    zstep(2)
    ring_b(zh, 0)
    ring_a_far(zh)
    zstep(3)
    rfull(slot_of(0, 0, other), zpart).wait_recv()
    begin(other)
    ring_b(zh, 1)
    ring_b(zh, 2)
    zstep(4)
    ring_a(other)
    ring_b(zh, 3)
    zstep(5)
    ring_b(other, 0)
    ring_a_far(other)
    zstep(6)
    ring_b(other, 1)
    ring_b(other, 2)
    zstep(7)
    ring_b(other, 3)
    zstep(8)
    for hh in (zh, other):
        for n in range(4):
            ring_b_far(hh, n)

    def pwait(slot, _):
        @pl.when(slot % 16 != x * 4 + y)
        def _():
            pltpu.make_async_remote_copy(
                src_ref=lb_ref.at[slot],
                dst_ref=lb_ref.at[slot],
                send_sem=psend.at[0],
                recv_sem=precv.at[slot],
                device_id=sib,
                device_id_type=MESH,
            ).wait_recv()

        return 0

    lax.fori_loop(0, 32, pwait, 0)
    for n in range(4):
        for m in range(4):
            lt_ref[m * 128 : (m + 1) * 128, n * 128 : (n + 1) * 128] = (
                lb_ref[n * 8 : (n + 1) * 8, :, m * 128 : (m + 1) * 128].reshape(128, 128).T
            )

    pltpu.make_async_remote_copy(
        src_ref=rb_ref.at[1 - core],
        dst_ref=rb_ref.at[1 - core],
        send_sem=sibsend.at[0],
        recv_sem=sibrecv.at[0],
        device_id=sib,
        device_id_type=MESH,
    ).wait_recv()

    for h in range(2):

        def outer(qb, _, h=h):
            off = pl.multiple_of(qb * 256, 256)
            right = rb_ref[h, :, :, pl.ds(off, 256)].reshape(512, 256)
            prod = jnp.dot(lt_ref[...], right, preferred_element_type=F32).astype(BF16)
            row = pl.multiple_of((h * 16 + qb * 2) * 32, 64)
            for i in range(16):
                for q in range(2):
                    oall_ref[
                        i // 2, pl.ds(row + q * 32, 32), (i % 2) * 128 : (i % 2 + 1) * 128
                    ] = prod[i * 32 : (i + 1) * 32, q * 128 : (q + 1) * 128]
            return 0

        lax.fori_loop(0, 8, outer, 0)

    for load in loads[5:]:
        load.wait()
    gain2 = g2_ref[...]

    def finish(n, _):
        for m in range(2):
            up = jnp.dot(wt_ref[...], oall_ref[n * 2 + m], preferred_element_type=F32)
            mids = []
            for k in range(2):
                i = n * 4 + m * 2 + k
                mids.append(
                    cpl_ref[i].astype(F32) + up[:, k * 128 : (k + 1) * 128].T * (1.0 / 512.0)
                )
            mid = jnp.concatenate(mids, axis=0)
            mean = jnp.mean(mid, axis=-1, keepdims=True)
            cen = mid - mean
            var = jnp.mean(cen * cen, axis=-1, keepdims=True)
            normed = (cen * lax.rsqrt(var + EPS) * gain2).astype(BF16)
            hidden = jnp.maximum(
                jnp.dot(normed, wa_ref[...], preferred_element_type=F32), 0.0
            ).astype(BF16)
            res = mid + jnp.dot(hidden, wb_ref[...], preferred_element_type=F32)
            out_ref[pl.ds(n * 4 + m * 2, 2)] = res.astype(BF16).reshape(2, 128, 128)
        return 0

    lax.fori_loop(0, 4, finish, 0)

    swap(0).wait_send()
    swap(1).wait_send()
    for ref, sem in (
        (rb_ref.at[core, pl.ds(0, 31)], rsend),
        (rb_ref.at[core], sibsend),
        (lb_ref.at[pl.ds(0, 30)], psend),
    ):
        pltpu.make_async_remote_copy(
            src_ref=ref,
            dst_ref=ref,
            send_sem=sem.at[0],
            recv_sem=sibrecv.at[0],
            device_id=sib,
            device_id_type=MESH,
        ).wait_send()
    for d in range(8):
        zforward(0, d, sent)
        if d < 7:
            zforward(1, d, sent)


def on_device(x, cpl, g1, w1, w2, w3, g2, wa, wb):
    vmem = pl.BlockSpec(memory_space=pltpu.VMEM)
    hbm = pl.BlockSpec(memory_space=pl.ANY)
    dma = pltpu.SemaphoreType.DMA
    args = (x, cpl, g1.reshape(1, 256), w1.T, w2.T, w3, g2.reshape(1, 128), wa, wb)
    return pl.pallas_call(
        kernel,
        out_shape=jax.ShapeDtypeStruct(cpl.shape, BF16),
        in_specs=[hbm] * len(args),
        out_specs=vmem,
        scratch_shapes=[pltpu.VMEM(a.shape, a.dtype) for a in args]
        + [
            pltpu.VMEM((1024, 128), F32),
            pltpu.VMEM((128, 1024), BF16),
            pltpu.VMEM((1024, 256), BF16),
            pltpu.VMEM((1024, 128), F32),
            pltpu.VMEM((2, 4, 8, 512), F32),
            pltpu.VMEM((256, 128), F32),
            pltpu.VMEM((2, 4, 8, 512), F32),
            pltpu.VMEM((2, 128, 128), F32),
            pltpu.VMEM((16, 2, 2, 16, 512), BF16),
            pltpu.VMEM((32, 16, 512), BF16),
            pltpu.VMEM((512, 512), BF16),
            pltpu.VMEM((2, 32, 16, 2048), BF16),
            pltpu.VMEM((8, 1024, 256), BF16),
            dma((len(args),)),
            dma((2,)),
            dma((2,)),
            dma((1,)),
            dma((32, 2)),
            dma((1,)),
            dma((1,)),
            dma((2, 8, 2)),
            dma((16, 2)),
            dma((1,)),
            dma((32,)),
        ],
        compiler_params=pltpu.CompilerParams(
            collective_id=0, has_side_effects=True, vmem_limit_bytes=66000000
        ),
    )(*args)


def solution(mesh):
    return jax.shard_map(
        on_device,
        mesh=mesh,
        in_specs=(
            P("rows", "cols", None),
            P("rows", "cols", None),
            P(),
            P(),
            P(),
            P(),
            P(),
            P(),
            P(),
        ),
        out_specs=P("rows", "cols", None),
        check_vma=False,
    )
```

```python
import jax
import jax.numpy as jnp
from jax import lax
from jax.experimental import pallas as pl
from jax.experimental.pallas import tpu as pltpu
from jax.sharding import PartitionSpec as P

MESH = pl.DeviceIdType.MESH
F32 = jnp.float32
BF16 = jnp.bfloat16
EPS = 1e-5


def kernel(
    x_hbm,
    cpl_hbm,
    g1_hbm,
    w1_hbm,
    w2_hbm,
    w3_hbm,
    g2_hbm,
    wa_hbm,
    wb_hbm,
    out_hbm,
    x_ref,
    cpl_ref,
    g1_ref,
    w1_ref,
    w2_ref,
    w3_ref,
    g2_ref,
    wa_ref,
    wb_ref,
    w3f_ref,
    wt_ref,
    xn_ref,
    tf_ref,
    lx_ref,
    rx_ref,
    xl_ref,
    xr_ref,
    lz_ref,
    lb_ref,
    lt_ref,
    rb_ref,
    ry_ref,
    oall_ref,
    mid_ref,
    nrm_ref,
    res_ref,
    in_sem,
    out_sem,
    xsend,
    xrecv,
    rsend,
    rrecv,
    sibsend,
    sibrecv,
    rysend,
    ryrecv,
    zsend,
    zrecv,
    psend,
    precv,
):
    r = lax.axis_index("rows")
    zl = lax.axis_index("cols")
    core = r % 2
    zh = (r // 2) % 2
    y = (r // 4) % 4
    x = r // 16
    z = zh * 8 + zl

    loads = [
        pltpu.make_async_copy(src, dst, in_sem.at[n])
        for n, (src, dst) in enumerate(
            [
                (x_hbm, x_ref),
                (g1_hbm, g1_ref),
                (w1_hbm, w1_ref),
                (w2_hbm, w2_ref),
                (w3_hbm, w3_ref),
                (cpl_hbm, cpl_ref),
                (g2_hbm, g2_ref),
                (wa_hbm, wa_ref),
                (wb_hbm, wb_ref),
            ]
        )
    ]
    for load in loads:
        load.start()

    def rows_of(xx, yy, hh, kk):
        return ((xx * 4 + yy) * 2 + hh) * 2 + kk

    sib = (rows_of(x, y, zh, 1 - core), zl)

    def zdev(dz):
        zz = (z + dz + 16) % 16
        return (rows_of(x, y, zz // 8, core), zz % 8)

    barrier = pltpu.get_barrier_semaphore()
    pl.semaphore_signal(barrier, inc=1, device_id=sib, device_id_type=MESH)
    for dz in (1, -1, 4, -4):
        pl.semaphore_signal(barrier, inc=1, device_id=zdev(dz), device_id_type=MESH)

    def greet_plane(d, _):
        px = (x + d // 4) % 4
        py = (y + d % 4) % 4
        pl.semaphore_signal(
            barrier, inc=1, device_id=(rows_of(px, py, zh, core), zl), device_id_type=MESH
        )
        return 0

    lax.fori_loop(1, 16, greet_plane, 0)

    for load in loads[:4]:
        load.wait()
    gain = g1_ref[...]
    for s in range(8):
        xs = x_ref[s].astype(F32)
        mean = jnp.mean(xs, axis=-1, keepdims=True)
        cen = xs - mean
        var = jnp.mean(cen * cen, axis=-1, keepdims=True)
        xn_ref[s * 128 : (s + 1) * 128, :] = (cen * lax.rsqrt(var + EPS) * gain).astype(BF16)
    wcat = jnp.concatenate([w1_ref[...]] * 4 + [w2_ref[...]] * 4, axis=0)
    for s in range(8):
        both = lax.dot_general(
            xn_ref[s * 128 : (s + 1) * 128, :],
            wcat,
            (((1,), (1,)), ((), ())),
            preferred_element_type=F32,
        )
        tf_ref[pl.ds(s, 128, stride=8), :] = both[:, :128]
        right = both[:, 128:].T
        rx_ref[pl.ds(s, 32, stride=8), :] = right[:32]
    lane = lax.broadcasted_iota(jnp.int32, (8, 128), 1) // 32
    for kk in range(2):
        for hh in range(2):
            for yy in range(2):
                gg = yy * 4 + hh * 2 + kk
                for g in range(4):
                    base = (gg * 16 + g * 4) * 8
                    tile = tf_ref[base : base + 8, :]
                    for e in range(1, 4):
                        other = tf_ref[base + e * 8 : base + e * 8 + 8, :]
                        tile = jnp.where(lane == e, other, tile)
                    lx_ref[kk, hh * 2 + yy, :, g * 128 : (g + 1) * 128] = tile

    pl.semaphore_wait(barrier, 20)

    def swap(n):
        if n == 0:
            src, dst = rx_ref.at[pl.ds(pl.multiple_of((1 - core) * 128, 128), 128)], xr_ref.at[core]
        else:
            src, dst = lx_ref.at[1 - core], xl_ref.at[core]
        return pltpu.make_async_remote_copy(
            src_ref=src,
            dst_ref=dst,
            send_sem=xsend.at[n],
            recv_sem=xrecv.at[n],
            device_id=sib,
            device_id_type=MESH,
        )

    def swap_in(n):
        dst = xr_ref.at[1 - core] if n == 0 else xl_ref.at[1 - core]
        return pltpu.make_async_remote_copy(
            src_ref=dst,
            dst_ref=dst,
            send_sem=xsend.at[n],
            recv_sem=xrecv.at[n],
            device_id=sib,
            device_id_type=MESH,
        )

    swap(0).start()
    swap(1).start()
    xr_ref[core] = rx_ref[pl.ds(pl.multiple_of(core * 128, 128), 128), :]
    xl_ref[core] = lx_ref[core]

    def zmessage(way, d):
        last = 8 - way
        return (last,) if d < last else ()

    def half_of(zz):
        return ((zz + 32) % 16) // 8

    def zparts(way, origin, d):
        sgn = 1 - 2 * way
        part = half_of(origin + sgn * d)
        count = 0
        for e in zmessage(way, d):
            count = count + (half_of(origin + sgn * e) + part) % 2
        return part, count

    def zcopy(way, origin, part, d, hop):
        return pltpu.make_async_remote_copy(
            src_ref=lz_ref.at[origin, part],
            dst_ref=lz_ref.at[origin, part],
            send_sem=zsend.at[way, d, part],
            recv_sem=zrecv.at[origin, part],
            device_id=zdev(hop),
            device_id_type=MESH,
        )

    zfrom = {d: (d - 1, 1) for d in range(1, 9)}

    def zput(way, d, act):
        at_d, hop = zfrom[d]
        sgn = 1 - 2 * way
        origin = (z - sgn * at_d + 16) % 16
        part, count = zparts(way, origin, d)
        act(zcopy(way, origin, part, d, sgn * hop))
        if zmessage(way, d):

            @pl.when(count > 0)
            def _():
                act(zcopy(way, origin, 1 - part, d, sgn * hop))

    def zget(way, d):
        sgn = 1 - 2 * way
        origin = (z - sgn * d + 16) % 16
        part, count = zparts(way, origin, d)
        zcopy(way, origin, zh, d, 1).wait_recv()
        if zmessage(way, d):

            @pl.when(count > 0)
            def _():
                zcopy(way, origin, 1 - zh, d, 1).wait_recv()

        return origin

    def pcopy(origin, py2):
        cc = origin % 8
        return pltpu.make_async_remote_copy(
            src_ref=lz_ref.at[origin, zh, py2],
            dst_ref=lb_ref.at[(origin // 8) * 16 + x * 4 + y],
            send_sem=psend.at[0],
            recv_sem=precv.at[(origin // 8) * 16 + x * 4 + y],
            device_id=(rows_of(cc // 2, (cc % 2) * 2 + py2, zh, core), zl),
            device_id_type=MESH,
        )

    def spread(origin):
        cc = origin % 8

        def body(py2, _):
            here = jnp.logical_and(cc // 2 == x, (cc % 2) * 2 + py2 == y)

            @pl.when(here)
            def _():
                lb_ref[(origin // 8) * 16 + x * 4 + y] = lz_ref[origin, zh, py2]

            @pl.when(jnp.logical_not(here))
            def _():
                pcopy(origin, py2).start()

            return 0

        lax.fori_loop(0, 2, body, 0)

    def start(copy):
        copy.start()

    def sent(copy):
        copy.wait_send()

    mine = zh * 16 + x * 4 + y
    swap_in(0).wait_recv()
    for q in range(16):
        rb_ref[core, mine, :, q * 128 : (q + 1) * 128] = jnp.concatenate(
            [xr_ref[0, q * 8 : (q + 1) * 8, :], xr_ref[1, q * 8 : (q + 1) * 8, :]], axis=0
        ).astype(BF16)

    def at(da, db):
        px = (x + da * (1 - core) + db * core + 4) % 4
        py = (y + da * core + db * (1 - core) + 4) % 4
        return px, py

    def slot_of(da, db, hh):
        px, py = at(da, db)
        return hh * 16 + px * 4 + py

    def dev_of(da, db):
        px, py = at(da, db)
        return (rows_of(px, py, zh, core), zl)

    def rfull(slot, dev):
        return pltpu.make_async_remote_copy(
            src_ref=rb_ref.at[core, slot],
            dst_ref=rb_ref.at[core, slot],
            send_sem=rsend.at[0],
            recv_sem=rrecv.at[slot, 0],
            device_id=dev,
            device_id_type=MESH,
        )

    def rhalf(slot, part, dev):
        piece = rb_ref.at[core, slot, :, pl.ds(part * 1024, 1024)]
        return pltpu.make_async_remote_copy(
            src_ref=piece,
            dst_ref=piece,
            send_sem=rsend.at[0],
            recv_sem=rrecv.at[slot, part],
            device_id=dev,
            device_id_type=MESH,
        )

    def scopy(slot):
        return pltpu.make_async_remote_copy(
            src_ref=rb_ref.at[core, slot],
            dst_ref=rb_ref.at[core, slot],
            send_sem=sibsend.at[0],
            recv_sem=sibrecv.at[0],
            device_id=sib,
            device_id_type=MESH,
        )

    steps = (0, -1, 1, 2)

    def begin(hh):
        slot = slot_of(0, 0, hh)
        for da, db in ((1, 0), (-1, 0), (0, 1), (0, -1)):
            rfull(slot, dev_of(da, db)).start()
        scopy(slot).start()

    def to_b(slot):
        rfull(slot, dev_of(0, 1)).start()
        rfull(slot, dev_of(0, -1)).start()
        scopy(slot).start()

    def ring_a(hh):
        for part in range(2):
            step = 1 - 2 * part
            slot = slot_of(-step, 0, hh)
            rfull(slot, dev_of(step, 0)).wait_recv()
            rhalf(slot, part, dev_of(step, 0)).start()
            to_b(slot)

    def ring_a_far(hh):
        slot = slot_of(2, 0, hh)
        for part in range(2):
            rhalf(slot, part, dev_of(1, 0)).wait_recv()
        to_b(slot)

    def ring_b(hh, n):
        for part in range(2):
            step = 1 - 2 * part
            slot = slot_of(steps[n], -step, hh)
            rfull(slot, dev_of(0, step)).wait_recv()
            rhalf(slot, part, dev_of(0, step)).start()
            scopy(slot).start()

    def ring_b_far(hh, n):
        slot = slot_of(steps[n], 2, hh)
        for part in range(2):
            rhalf(slot, part, dev_of(0, 1)).wait_recv()
        scopy(slot).start()

    def begin_straight(hh):
        slot = slot_of(0, 0, hh)
        for step in (1, -1, 2):
            rfull(slot, dev_of(step, 0)).start()
        for step in (1, -1, 2):
            rfull(slot, dev_of(0, step)).start()
        scopy(slot).start()

    def ring_a_straight(hh):
        for da in (-1, 1, 2):
            slot = slot_of(da, 0, hh)
            rfull(slot, dev_of(1, 0)).wait_recv()
            for step in (1, -1, 2):
                rfull(slot, dev_of(0, step)).start()
            scopy(slot).start()

    def ring_b_straight(hh, n):
        for db in (-1, 1, 2):
            slot = slot_of(steps[n], db, hh)
            rfull(slot, dev_of(0, 1)).wait_recv()
            scopy(slot).start()

    theirs = slot_of(0, 0, 1 - zh)

    def rout(part):
        return pltpu.make_async_remote_copy(
            src_ref=rb_ref.at[core, mine, :, pl.ds(part * 1024, 1024)],
            dst_ref=ry_ref.at[part],
            send_sem=rysend.at[part],
            recv_sem=ryrecv.at[part],
            device_id=zdev(4 - 8 * part),
            device_id_type=MESH,
        )

    def ron(part):
        slot = half_of(z - 4 + 8 * part) * 16 + x * 4 + y
        return pltpu.make_async_remote_copy(
            src_ref=ry_ref.at[part],
            dst_ref=rb_ref.at[core, slot, :, pl.ds(part * 1024, 1024)],
            send_sem=rysend.at[2 + part],
            recv_sem=rrecv.at[slot, part],
            device_id=zdev(4 - 8 * part),
            device_id_type=MESH,
        )

    rout(0).start()
    rout(1).start()
    begin(zh)
    swap_in(1).wait_recv()
    for hy in range(4):
        for g in range(4):
            cols = slice(g * 128, (g + 1) * 128)
            lz_ref[z, hy // 2, hy % 2, :, cols] = jnp.concatenate(
                [xl_ref[0, hy, :, cols], xl_ref[1, hy, :, cols]], axis=0
            ).astype(BF16)
    for way in range(2):
        zput(way, 1, start)
    spread(z)

    loads[4].wait()
    for p in range(32):
        w3f_ref[pl.ds(p, 32, stride=32), :] = w3_ref[p * 32 : (p + 1) * 32, :].astype(F32)
    for n in range(8):
        wt_ref[:, n * 128 : (n + 1) * 128] = w3f_ref[n * 128 : (n + 1) * 128, :].T.astype(BF16)

    def zstep(d):
        ways = range(1 if d == 8 else 2)
        origins = []
        for way in ways:
            origins.append(zget(way, d))
            for nxt, (at_d, _) in zfrom.items():
                if at_d == d and nxt <= 8 - way:
                    zput(way, nxt, start)
        for origin in origins:
            spread(origin)

    other = 1 - zh
    ring_a(zh)
    ring_b(zh, 0)
    for part in range(2):
        rout(part).wait_recv()
        ron(part).start()
    zstep(1)
    ring_a_far(zh)
    zstep(2)
    ring_b(zh, 1)
    ring_b(zh, 2)
    zstep(3)
    for part in range(2):
        rhalf(theirs, part, dev_of(1, 0)).wait_recv()
    begin_straight(other)
    ring_b(zh, 3)
    zstep(4)
    ring_a_straight(other)
    zstep(5)
    for n in range(4):
        ring_b_far(zh, n)
    zstep(6)
    ring_b_straight(other, 0)
    zstep(7)
    ring_b_straight(other, 1)
    zstep(8)
    ring_b_straight(other, 2)
    ring_b_straight(other, 3)

    def pwait(slot, _):
        @pl.when(slot % 16 != x * 4 + y)
        def _():
            pltpu.make_async_remote_copy(
                src_ref=lb_ref.at[slot],
                dst_ref=lb_ref.at[slot],
                send_sem=psend.at[0],
                recv_sem=precv.at[slot],
                device_id=sib,
                device_id_type=MESH,
            ).wait_recv()

        return 0

    lax.fori_loop(0, 32, pwait, 0)
    for n in range(4):
        for m in range(4):
            lt_ref[m * 128 : (m + 1) * 128, n * 128 : (n + 1) * 128] = (
                lb_ref[n * 8 : (n + 1) * 8, :, m * 128 : (m + 1) * 128].reshape(128, 128).T
            )

    pltpu.make_async_remote_copy(
        src_ref=rb_ref.at[1 - core],
        dst_ref=rb_ref.at[1 - core],
        send_sem=sibsend.at[0],
        recv_sem=sibrecv.at[0],
        device_id=sib,
        device_id_type=MESH,
    ).wait_recv()

    for h in range(2):

        def outer(qb, _, h=h):
            off = pl.multiple_of(qb * 512, 512)
            right = rb_ref[h, :, :, pl.ds(off, 512)].reshape(512, 512)
            prod = jnp.dot(lt_ref[...], right, preferred_element_type=F32).astype(BF16)
            row = pl.multiple_of((h * 16 + qb * 4) * 32, 128)
            for i in range(16):
                for q in range(4):
                    oall_ref[
                        i // 2, pl.ds(row + q * 32, 32), (i % 2) * 128 : (i % 2 + 1) * 128
                    ] = prod[i * 32 : (i + 1) * 32, q * 128 : (q + 1) * 128]
            return 0

        lax.fori_loop(0, 4, outer, 0)

    for load in loads[5:]:
        load.wait()
    gain2 = g2_ref[...]

    def contract(n, _):
        for m in range(4):
            up = jnp.dot(wt_ref[...], oall_ref[n * 4 + m], preferred_element_type=F32)
            for k in range(2):
                i = n * 8 + m * 2 + k
                mid_ref[i] = cpl_ref[i].astype(F32) + up[:, k * 128 : (k + 1) * 128].T * (
                    1.0 / 512.0
                )
        return 0

    lax.fori_loop(0, 2, contract, 0)

    def norm_pair(n, _):
        mid = mid_ref[pl.ds(n * 4, 4)].reshape(512, 128)
        mean = jnp.mean(mid, axis=-1, keepdims=True)
        cen = mid - mean
        var = jnp.mean(cen * cen, axis=-1, keepdims=True)
        nrm_ref[n] = (cen * lax.rsqrt(var + EPS) * gain2).astype(BF16)
        return 0

    lax.fori_loop(0, 4, norm_pair, 0)

    def result(n):
        return pltpu.make_async_copy(
            res_ref.at[pl.ds(n * 4, 4)], out_hbm.at[pl.ds(n * 4, 4)], out_sem.at[n]
        )

    def transition(n, _):
        hidden = jnp.maximum(
            jnp.dot(nrm_ref[n], wa_ref[...], preferred_element_type=F32), 0.0
        ).astype(BF16)
        res = mid_ref[pl.ds(n * 4, 4)].reshape(512, 128) + jnp.dot(
            hidden, wb_ref[...], preferred_element_type=F32
        )
        res_ref[pl.ds(n * 4, 4)] = res.astype(BF16).reshape(4, 128, 128)
        result(n).start()
        return 0

    lax.fori_loop(0, 4, transition, 0)

    swap(0).wait_send()
    swap(1).wait_send()
    for ref, sem in (
        (rb_ref.at[core, pl.ds(0, 30)], rsend),
        (rb_ref.at[core], sibsend),
        (lb_ref.at[pl.ds(0, 30)], psend),
    ):
        pltpu.make_async_remote_copy(
            src_ref=ref,
            dst_ref=ref,
            send_sem=sem.at[0],
            recv_sem=sibrecv.at[0],
            device_id=sib,
            device_id_type=MESH,
        ).wait_send()
    for part in range(2):
        rout(part).wait_send()
        ron(part).wait_send()
    for d in range(1, 9):
        for way in range(1 if d == 8 else 2):
            zput(way, d, sent)
    for n in range(4):
        result(n).wait()


def on_device(x, cpl, g1, w1, w2, w3, g2, wa, wb):
    hbm = pl.BlockSpec(memory_space=pltpu.HBM)
    dma = pltpu.SemaphoreType.DMA
    args = (x, cpl, g1.reshape(1, 256), w1.T, w2.T, w3, g2.reshape(1, 128), wa, wb)
    return pl.pallas_call(
        kernel,
        out_shape=jax.ShapeDtypeStruct(cpl.shape, BF16),
        in_specs=[hbm] * len(args),
        out_specs=hbm,
        scratch_shapes=[pltpu.VMEM(a.shape, a.dtype) for a in args]
        + [
            pltpu.VMEM((1024, 128), F32),
            pltpu.VMEM((128, 1024), BF16),
            pltpu.VMEM((1024, 256), BF16),
            pltpu.VMEM((1024, 128), F32),
            pltpu.VMEM((2, 4, 8, 512), F32),
            pltpu.VMEM((256, 128), F32),
            pltpu.VMEM((2, 4, 8, 512), F32),
            pltpu.VMEM((2, 128, 128), F32),
            pltpu.VMEM((16, 2, 2, 16, 512), BF16),
            pltpu.VMEM((32, 16, 512), BF16),
            pltpu.VMEM((512, 512), BF16),
            pltpu.VMEM((2, 32, 16, 2048), BF16),
            pltpu.VMEM((2, 16, 1024), BF16),
            pltpu.VMEM((8, 1024, 256), BF16),
            pltpu.VMEM((16, 128, 128), F32),
            pltpu.VMEM((4, 512, 128), BF16),
            pltpu.VMEM((16, 128, 128), BF16),
            dma((len(args),)),
            dma((4,)),
            dma((2,)),
            dma((2,)),
            dma((1,)),
            dma((32, 2)),
            dma((1,)),
            dma((1,)),
            dma((4,)),
            dma((2,)),
            dma((2, 9, 2)),
            dma((16, 2)),
            dma((1,)),
            dma((32,)),
        ],
        compiler_params=pltpu.CompilerParams(
            collective_id=0, has_side_effects=True, vmem_limit_bytes=66500000
        ),
    )(*args)


def solution(mesh):
    return jax.shard_map(
        on_device,
        mesh=mesh,
        in_specs=(
            P("rows", "cols", None),
            P("rows", "cols", None),
            P(),
            P(),
            P(),
            P(),
            P(),
            P(),
            P(),
        ),
        out_specs=P("rows", "cols", None),
        check_vma=False,
    )
```

```python
import jax
import jax.numpy as jnp
from jax import lax
from jax.experimental import pallas as pl
from jax.experimental.pallas import tpu as pltpu
from jax.sharding import PartitionSpec as P

MESH = pl.DeviceIdType.MESH
F32 = jnp.float32
BF16 = jnp.bfloat16
EPS = 1e-5


def kernel(
    x_hbm,
    cpl_hbm,
    g1_hbm,
    w1_hbm,
    w2_hbm,
    w3_hbm,
    g2_hbm,
    wa_hbm,
    wb_hbm,
    out_hbm,
    x_ref,
    cpl_ref,
    g1_ref,
    w1_ref,
    w2_ref,
    w3_ref,
    g2_ref,
    wa_ref,
    wb_ref,
    w3f_ref,
    wt_ref,
    xn_ref,
    tf_ref,
    lx_ref,
    rx_ref,
    xl_ref,
    xr_ref,
    lz_ref,
    lb_ref,
    lt_ref,
    rb_ref,
    ry_ref,
    oall_ref,
    mid_ref,
    nrm_ref,
    res_ref,
    in_sem,
    out_sem,
    xsend,
    xrecv,
    rsend,
    rrecv,
    sibsend,
    sibrecv,
    rysend,
    ryrecv,
    zsend,
    zrecv,
    psend,
    precv,
):
    r = lax.axis_index("rows")
    zl = lax.axis_index("cols")
    core = r % 2
    zh = (r // 2) % 2
    y = (r // 4) % 4
    x = r // 16
    z = zh * 8 + zl

    loads = [
        pltpu.make_async_copy(src, dst, in_sem.at[n])
        for n, (src, dst) in enumerate(
            [
                (x_hbm, x_ref),
                (g1_hbm, g1_ref),
                (w1_hbm, w1_ref),
                (w2_hbm, w2_ref),
                (w3_hbm, w3_ref),
                (cpl_hbm, cpl_ref),
                (g2_hbm, g2_ref),
                (wa_hbm, wa_ref),
                (wb_hbm, wb_ref),
            ]
        )
    ]
    for load in loads:
        load.start()

    def rows_of(xx, yy, hh, kk):
        return ((xx * 4 + yy) * 2 + hh) * 2 + kk

    sib = (rows_of(x, y, zh, 1 - core), zl)

    def zdev(dz):
        zz = (z + dz + 16) % 16
        return (rows_of(x, y, zz // 8, core), zz % 8)

    barrier = pltpu.get_barrier_semaphore()
    pl.semaphore_signal(barrier, inc=1, device_id=sib, device_id_type=MESH)
    for dz in (1, -1, 4, -4):
        pl.semaphore_signal(barrier, inc=1, device_id=zdev(dz), device_id_type=MESH)

    def greet_plane(d, _):
        px = (x + d // 4) % 4
        py = (y + d % 4) % 4
        pl.semaphore_signal(
            barrier, inc=1, device_id=(rows_of(px, py, zh, core), zl), device_id_type=MESH
        )
        return 0

    lax.fori_loop(1, 16, greet_plane, 0)

    for load in loads[:4]:
        load.wait()
    gain = g1_ref[...]
    for s in range(8):
        xs = x_ref[s].astype(F32)
        mean = jnp.mean(xs, axis=-1, keepdims=True)
        cen = xs - mean
        var = jnp.mean(cen * cen, axis=-1, keepdims=True)
        xn_ref[s * 128 : (s + 1) * 128, :] = (cen * lax.rsqrt(var + EPS) * gain).astype(BF16)
    wcat = jnp.concatenate([w1_ref[...]] * 4 + [w2_ref[...]] * 4, axis=0)
    for s in range(8):
        both = lax.dot_general(
            xn_ref[s * 128 : (s + 1) * 128, :],
            wcat,
            (((1,), (1,)), ((), ())),
            preferred_element_type=F32,
        )
        tf_ref[pl.ds(s, 128, stride=8), :] = both[:, :128]
        right = both[:, 128:].T
        rx_ref[pl.ds(s, 32, stride=8), :] = right[:32]
    lane = lax.broadcasted_iota(jnp.int32, (8, 128), 1) // 32
    for kk in range(2):
        for hh in range(2):
            for yy in range(2):
                gg = yy * 4 + hh * 2 + kk
                for g in range(4):
                    base = (gg * 16 + g * 4) * 8
                    tile = tf_ref[base : base + 8, :]
                    for e in range(1, 4):
                        other = tf_ref[base + e * 8 : base + e * 8 + 8, :]
                        tile = jnp.where(lane == e, other, tile)
                    lx_ref[kk, hh * 2 + yy, :, g * 128 : (g + 1) * 128] = tile

    pl.semaphore_wait(barrier, 20)

    def swap(n):
        if n == 0:
            src, dst = rx_ref.at[pl.ds(pl.multiple_of((1 - core) * 128, 128), 128)], xr_ref.at[core]
        else:
            src, dst = lx_ref.at[1 - core], xl_ref.at[core]
        return pltpu.make_async_remote_copy(
            src_ref=src,
            dst_ref=dst,
            send_sem=xsend.at[n],
            recv_sem=xrecv.at[n],
            device_id=sib,
            device_id_type=MESH,
        )

    def swap_in(n):
        dst = xr_ref.at[1 - core] if n == 0 else xl_ref.at[1 - core]
        return pltpu.make_async_remote_copy(
            src_ref=dst,
            dst_ref=dst,
            send_sem=xsend.at[n],
            recv_sem=xrecv.at[n],
            device_id=sib,
            device_id_type=MESH,
        )

    swap(0).start()
    swap(1).start()
    xr_ref[core] = rx_ref[pl.ds(pl.multiple_of(core * 128, 128), 128), :]
    xl_ref[core] = lx_ref[core]

    def zmessage(way, d):
        last = 8 - way
        return (last,) if d < last else ()

    def half_of(zz):
        return ((zz + 32) % 16) // 8

    def zparts(way, origin, d):
        sgn = 1 - 2 * way
        part = half_of(origin + sgn * d)
        count = 0
        for e in zmessage(way, d):
            count = count + (half_of(origin + sgn * e) + part) % 2
        return part, count

    def zcopy(way, origin, part, d, hop):
        piece = lz_ref.at[origin] if part is None else lz_ref.at[origin, part]
        return pltpu.make_async_remote_copy(
            src_ref=piece,
            dst_ref=piece,
            send_sem=zsend.at[way, d],
            recv_sem=zrecv.at[origin],
            device_id=zdev(hop),
            device_id_type=MESH,
        )

    def zeither(way, origin, part, count, d, hop, act):
        if not zmessage(way, d):
            act(zcopy(way, origin, part, d, hop))
            return

        @pl.when(count > 0)
        def _():
            act(zcopy(way, origin, None, d, hop))

        @pl.when(count == 0)
        def _():
            act(zcopy(way, origin, part, d, hop))

    zfrom = {d: (d - 1, 1) for d in range(1, 9)}

    def zput(way, d, act):
        at_d, hop = zfrom[d]
        sgn = 1 - 2 * way
        origin = (z - sgn * at_d + 16) % 16
        part, count = zparts(way, origin, d)
        zeither(way, origin, part, count, d, sgn * hop, act)

    def zget(way, d):
        sgn = 1 - 2 * way
        origin = (z - sgn * d + 16) % 16
        part, count = zparts(way, origin, d)
        zeither(way, origin, zh, count, d, 1, lambda copy: copy.wait_recv())
        return origin

    def pcopy(origin, py2):
        cc = origin % 8
        return pltpu.make_async_remote_copy(
            src_ref=lz_ref.at[origin, zh, py2],
            dst_ref=lb_ref.at[(origin // 8) * 16 + x * 4 + y],
            send_sem=psend.at[0],
            recv_sem=precv.at[0],
            device_id=(rows_of(cc // 2, (cc % 2) * 2 + py2, zh, core), zl),
            device_id_type=MESH,
        )

    def spread(origin):
        cc = origin % 8

        def body(py2, _):
            here = jnp.logical_and(cc // 2 == x, (cc % 2) * 2 + py2 == y)

            @pl.when(here)
            def _():
                lb_ref[(origin // 8) * 16 + x * 4 + y] = lz_ref[origin, zh, py2]

            @pl.when(jnp.logical_not(here))
            def _():
                pcopy(origin, py2).start()

            return 0

        lax.fori_loop(0, 2, body, 0)

    def start(copy):
        copy.start()

    def sent(copy):
        copy.wait_send()

    mine = zh * 16 + x * 4 + y
    swap_in(0).wait_recv()
    for q in range(16):
        rb_ref[core, mine, :, q * 128 : (q + 1) * 128] = jnp.concatenate(
            [xr_ref[0, q * 8 : (q + 1) * 8, :], xr_ref[1, q * 8 : (q + 1) * 8, :]], axis=0
        ).astype(BF16)

    def at(da, db):
        px = (x + da * (1 - core) + db * core + 4) % 4
        py = (y + da * core + db * (1 - core) + 4) % 4
        return px, py

    def slot_of(da, db, hh):
        px, py = at(da, db)
        return hh * 16 + px * 4 + py

    def dev_of(da, db):
        px, py = at(da, db)
        return (rows_of(px, py, zh, core), zl)

    def rblocks(count, sem):
        return pltpu.make_async_remote_copy(
            src_ref=rb_ref.at[core, pl.ds(0, count)],
            dst_ref=rb_ref.at[core, pl.ds(0, count)],
            send_sem=rsend.at[0],
            recv_sem=rrecv.at[sem],
            device_id=sib,
            device_id_type=MESH,
        )

    def rfull(slot, dev, sem):
        return pltpu.make_async_remote_copy(
            src_ref=rb_ref.at[core, slot],
            dst_ref=rb_ref.at[core, slot],
            send_sem=rsend.at[0],
            recv_sem=rrecv.at[sem],
            device_id=dev,
            device_id_type=MESH,
        )

    def rhalf(slot, part, dev, sem):
        piece = rb_ref.at[core, slot, :, pl.ds(part * 1024, 1024)]
        return pltpu.make_async_remote_copy(
            src_ref=piece,
            dst_ref=piece,
            send_sem=rsend.at[0],
            recv_sem=rrecv.at[sem],
            device_id=dev,
            device_id_type=MESH,
        )

    def scopy(slot):
        return pltpu.make_async_remote_copy(
            src_ref=rb_ref.at[core, slot],
            dst_ref=rb_ref.at[core, slot],
            send_sem=sibsend.at[0],
            recv_sem=sibrecv.at[0],
            device_id=sib,
            device_id_type=MESH,
        )

    steps = (0, -1, 1, 2)

    def begin(hh):
        slot = slot_of(0, 0, hh)
        for da, db, sem in ((1, 0, 0), (-1, 0, 1), (0, 1, 3), (0, -1, 4)):
            rfull(slot, dev_of(da, db), sem).start()
        scopy(slot).start()

    def to_b(slot, n):
        rfull(slot, dev_of(0, 1), 3 + 2 * n).start()
        rfull(slot, dev_of(0, -1), 4 + 2 * n).start()
        scopy(slot).start()

    def ring_a(hh):
        for part in range(2):
            step = 1 - 2 * part
            slot = slot_of(-step, 0, hh)
            rblocks(1, part).wait_recv()
            rhalf(slot, part, dev_of(step, 0), 2).start()
            to_b(slot, 1 + part)

    def ring_a_far(hh):
        rblocks(1, 2).wait_recv()
        to_b(slot_of(2, 0, hh), 3)

    def ring_b(hh, n):
        for part in range(2):
            step = 1 - 2 * part
            slot = slot_of(steps[n], -step, hh)
            rblocks(1, 3 + 2 * n + part).wait_recv()
            rhalf(slot, part, dev_of(0, step), 11).start()
            scopy(slot).start()

    def ring_b_far(hh):
        rblocks(4, 11).wait_recv()
        for n in range(4):
            scopy(slot_of(steps[n], 2, hh)).start()

    def begin_straight(hh):
        slot = slot_of(0, 0, hh)
        for step, sem in ((1, 13), (-1, 14), (2, 15)):
            rfull(slot, dev_of(step, 0), sem).start()
        for step in (1, -1, 2):
            rfull(slot, dev_of(0, step), 16).start()
        scopy(slot).start()

    def ring_a_straight(hh):
        for n in range(1, 4):
            slot = slot_of(steps[n], 0, hh)
            rblocks(1, 12 + n).wait_recv()
            for step in (1, -1, 2):
                rfull(slot, dev_of(0, step), 16 + n).start()
            scopy(slot).start()

    def ring_b_straight(hh, n):
        rblocks(3, 16 + n).wait_recv()
        for db in (-1, 1, 2):
            scopy(slot_of(steps[n], db, hh)).start()


    def rout(part):
        return pltpu.make_async_remote_copy(
            src_ref=rb_ref.at[core, mine, :, pl.ds(part * 1024, 1024)],
            dst_ref=ry_ref.at[part],
            send_sem=rysend.at[part],
            recv_sem=ryrecv.at[part],
            device_id=zdev(4 - 8 * part),
            device_id_type=MESH,
        )

    def ron(part):
        slot = half_of(z - 4 + 8 * part) * 16 + x * 4 + y
        return pltpu.make_async_remote_copy(
            src_ref=ry_ref.at[part],
            dst_ref=rb_ref.at[core, slot, :, pl.ds(part * 1024, 1024)],
            send_sem=rysend.at[2 + part],
            recv_sem=rrecv.at[12],
            device_id=zdev(4 - 8 * part),
            device_id_type=MESH,
        )

    rout(0).start()
    rout(1).start()
    begin(zh)
    swap_in(1).wait_recv()
    for hy in range(4):
        for g in range(4):
            cols = slice(g * 128, (g + 1) * 128)
            lz_ref[z, hy // 2, hy % 2, :, cols] = jnp.concatenate(
                [xl_ref[0, hy, :, cols], xl_ref[1, hy, :, cols]], axis=0
            ).astype(BF16)
    for way in range(2):
        zput(way, 1, start)
    spread(z)

    loads[4].wait()
    for p in range(32):
        w3f_ref[pl.ds(p, 32, stride=32), :] = w3_ref[p * 32 : (p + 1) * 32, :].astype(F32)
    for n in range(8):
        wt_ref[:, n * 128 : (n + 1) * 128] = w3f_ref[n * 128 : (n + 1) * 128, :].T.astype(BF16)

    def zstep(d):
        ways = range(1 if d == 8 else 2)
        origins = []
        for way in ways:
            origins.append(zget(way, d))
            for nxt, (at_d, _) in zfrom.items():
                if at_d == d and nxt <= 8 - way:
                    zput(way, nxt, start)
        for origin in origins:
            spread(origin)

    other = 1 - zh
    ring_a(zh)
    ring_b(zh, 0)
    for part in range(2):
        rout(part).wait_recv()
        ron(part).start()
    zstep(1)
    ring_a_far(zh)
    zstep(2)
    ring_b(zh, 1)
    ring_b(zh, 2)
    zstep(3)
    rblocks(1, 12).wait_recv()
    begin_straight(other)
    ring_b(zh, 3)
    zstep(4)
    ring_a_straight(other)
    zstep(5)
    ring_b_far(zh)
    zstep(6)
    ring_b_straight(other, 0)
    zstep(7)
    ring_b_straight(other, 1)
    zstep(8)
    ring_b_straight(other, 2)
    ring_b_straight(other, 3)

    pltpu.make_async_remote_copy(
        src_ref=lb_ref.at[pl.ds(0, 30)],
        dst_ref=lb_ref.at[pl.ds(0, 30)],
        send_sem=psend.at[0],
        recv_sem=precv.at[0],
        device_id=sib,
        device_id_type=MESH,
    ).wait_recv()
    for n in range(4):
        for m in range(4):
            lt_ref[m * 128 : (m + 1) * 128, n * 128 : (n + 1) * 128] = (
                lb_ref[n * 8 : (n + 1) * 8, :, m * 128 : (m + 1) * 128].reshape(128, 128).T
            )

    pltpu.make_async_remote_copy(
        src_ref=rb_ref.at[1 - core],
        dst_ref=rb_ref.at[1 - core],
        send_sem=sibsend.at[0],
        recv_sem=sibrecv.at[0],
        device_id=sib,
        device_id_type=MESH,
    ).wait_recv()

    for h in range(2):

        def outer(qb, _, h=h):
            off = pl.multiple_of(qb * 512, 512)
            right = rb_ref[h, :, :, pl.ds(off, 512)].reshape(512, 512)
            prod = jnp.dot(lt_ref[...], right, preferred_element_type=F32).astype(BF16)
            row = pl.multiple_of((h * 16 + qb * 4) * 32, 128)
            for i in range(16):
                for q in range(4):
                    oall_ref[
                        i // 2, pl.ds(row + q * 32, 32), (i % 2) * 128 : (i % 2 + 1) * 128
                    ] = prod[i * 32 : (i + 1) * 32, q * 128 : (q + 1) * 128]
            return 0

        lax.fori_loop(0, 4, outer, 0)

    for load in loads[5:]:
        load.wait()
    gain2 = g2_ref[...]

    def contract(n, _):
        for m in range(4):
            up = jnp.dot(wt_ref[...], oall_ref[n * 4 + m], preferred_element_type=F32)
            for k in range(2):
                i = n * 8 + m * 2 + k
                mid_ref[i] = cpl_ref[i].astype(F32) + up[:, k * 128 : (k + 1) * 128].T * (
                    1.0 / 512.0
                )
        return 0

    lax.fori_loop(0, 2, contract, 0)

    def norm_pair(n, _):
        mid = mid_ref[pl.ds(n * 4, 4)].reshape(512, 128)
        mean = jnp.mean(mid, axis=-1, keepdims=True)
        cen = mid - mean
        var = jnp.mean(cen * cen, axis=-1, keepdims=True)
        nrm_ref[n] = (cen * lax.rsqrt(var + EPS) * gain2).astype(BF16)
        return 0

    lax.fori_loop(0, 4, norm_pair, 0)

    def result(n):
        return pltpu.make_async_copy(
            res_ref.at[pl.ds(n * 4, 4)], out_hbm.at[pl.ds(n * 4, 4)], out_sem.at[n]
        )

    def transition(n, _):
        hidden = jnp.maximum(
            jnp.dot(nrm_ref[n], wa_ref[...], preferred_element_type=F32), 0.0
        ).astype(BF16)
        res = mid_ref[pl.ds(n * 4, 4)].reshape(512, 128) + jnp.dot(
            hidden, wb_ref[...], preferred_element_type=F32
        )
        res_ref[pl.ds(n * 4, 4)] = res.astype(BF16).reshape(4, 128, 128)
        result(n).start()
        return 0

    lax.fori_loop(0, 4, transition, 0)

    swap(0).wait_send()
    swap(1).wait_send()
    for ref, sem in (
        (rb_ref.at[core, pl.ds(0, 30)], rsend),
        (rb_ref.at[core], sibsend),
        (lb_ref.at[pl.ds(0, 30)], psend),
    ):
        pltpu.make_async_remote_copy(
            src_ref=ref,
            dst_ref=ref,
            send_sem=sem.at[0],
            recv_sem=sibrecv.at[0],
            device_id=sib,
            device_id_type=MESH,
        ).wait_send()
    for part in range(2):
        rout(part).wait_send()
        ron(part).wait_send()
    for d in range(1, 9):
        for way in range(1 if d == 8 else 2):
            zput(way, d, sent)
    for n in range(4):
        result(n).wait()


def on_device(x, cpl, g1, w1, w2, w3, g2, wa, wb):
    hbm = pl.BlockSpec(memory_space=pltpu.HBM)
    dma = pltpu.SemaphoreType.DMA
    args = (x, cpl, g1.reshape(1, 256), w1.T, w2.T, w3, g2.reshape(1, 128), wa, wb)
    return pl.pallas_call(
        kernel,
        out_shape=jax.ShapeDtypeStruct(cpl.shape, BF16),
        in_specs=[hbm] * len(args),
        out_specs=hbm,
        scratch_shapes=[pltpu.VMEM(a.shape, a.dtype) for a in args]
        + [
            pltpu.VMEM((1024, 128), F32),
            pltpu.VMEM((128, 1024), BF16),
            pltpu.VMEM((1024, 256), BF16),
            pltpu.VMEM((1024, 128), F32),
            pltpu.VMEM((2, 4, 8, 512), F32),
            pltpu.VMEM((256, 128), F32),
            pltpu.VMEM((2, 4, 8, 512), F32),
            pltpu.VMEM((2, 128, 128), F32),
            pltpu.VMEM((16, 2, 2, 16, 512), BF16),
            pltpu.VMEM((32, 16, 512), BF16),
            pltpu.VMEM((512, 512), BF16),
            pltpu.VMEM((2, 32, 16, 2048), BF16),
            pltpu.VMEM((2, 16, 1024), BF16),
            pltpu.VMEM((8, 1024, 256), BF16),
            pltpu.VMEM((16, 128, 128), F32),
            pltpu.VMEM((4, 512, 128), BF16),
            pltpu.VMEM((16, 128, 128), BF16),
            dma((len(args),)),
            dma((4,)),
            dma((2,)),
            dma((2,)),
            dma((1,)),
            dma((20,)),
            dma((1,)),
            dma((1,)),
            dma((4,)),
            dma((2,)),
            dma((2, 9)),
            dma((16,)),
            dma((1,)),
            dma((1,)),
        ],
        compiler_params=pltpu.CompilerParams(
            collective_id=0, has_side_effects=True, vmem_limit_bytes=66500000
        ),
    )(*args)


def solution(mesh):
    return jax.shard_map(
        on_device,
        mesh=mesh,
        in_specs=(
            P("rows", "cols", None),
            P("rows", "cols", None),
            P(),
            P(),
            P(),
            P(),
            P(),
            P(),
            P(),
        ),
        out_specs=P("rows", "cols", None),
        check_vma=False,
    )
```

```python
import jax
import jax.numpy as jnp
from jax import lax
from jax.experimental import pallas as pl
from jax.experimental.pallas import tpu as pltpu
from jax.sharding import PartitionSpec as P

MESH = pl.DeviceIdType.MESH
F32 = jnp.float32
BF16 = jnp.bfloat16
EPS = 1e-5


def kernel(
    x_hbm,
    cpl_hbm,
    g1_hbm,
    w1_hbm,
    w2_hbm,
    w3_hbm,
    g2_hbm,
    wa_hbm,
    wb_hbm,
    out_hbm,
    x_ref,
    cpl_ref,
    g1_ref,
    w1_ref,
    w2_ref,
    w3_ref,
    g2_ref,
    wa_ref,
    wb_ref,
    w3f_ref,
    wt_ref,
    xn_ref,
    tf_ref,
    lx_ref,
    rx_ref,
    xl_ref,
    xr_ref,
    lz_ref,
    lb_ref,
    lt_ref,
    rb_ref,
    ry_ref,
    oall_ref,
    mid_ref,
    nrm_ref,
    res_ref,
    in_sem,
    out_sem,
    xsend,
    xrecv,
    rsend,
    rrecv,
    sibsend,
    sibrecv,
    rysend,
    ryrecv,
    zsend,
    zrecv,
    psend,
    precv,
):
    r = lax.axis_index("rows")
    zl = lax.axis_index("cols")
    core = r % 2
    zh = (r // 2) % 2
    y = (r // 4) % 4
    x = r // 16
    z = zh * 8 + zl

    loads = [
        pltpu.make_async_copy(src, dst, in_sem.at[n])
        for n, (src, dst) in enumerate(
            [
                (x_hbm, x_ref),
                (g1_hbm, g1_ref),
                (w1_hbm, w1_ref),
                (w2_hbm, w2_ref),
                (w3_hbm, w3_ref),
                (cpl_hbm, cpl_ref),
                (g2_hbm, g2_ref),
                (wa_hbm, wa_ref),
                (wb_hbm, wb_ref),
            ]
        )
    ]
    for load in loads:
        load.start()

    def rows_of(xx, yy, hh, kk):
        return ((xx * 4 + yy) * 2 + hh) * 2 + kk

    sib = (rows_of(x, y, zh, 1 - core), zl)

    def zdev(dz):
        zz = (z + dz + 16) % 16
        return (rows_of(x, y, zz // 8, core), zz % 8)

    barrier = pltpu.get_barrier_semaphore()
    pl.semaphore_signal(barrier, inc=1, device_id=sib, device_id_type=MESH)
    for dz in (1, -1, 4, -4):
        pl.semaphore_signal(barrier, inc=1, device_id=zdev(dz), device_id_type=MESH)

    def greet_plane(d, _):
        px = (x + d // 4) % 4
        py = (y + d % 4) % 4
        pl.semaphore_signal(
            barrier, inc=1, device_id=(rows_of(px, py, zh, core), zl), device_id_type=MESH
        )
        return 0

    lax.fori_loop(1, 16, greet_plane, 0)

    for load in loads[:4]:
        load.wait()
    gain = g1_ref[...]
    for s in range(8):
        xs = x_ref[s].astype(F32)
        mean = jnp.mean(xs, axis=-1, keepdims=True)
        cen = xs - mean
        var = jnp.mean(cen * cen, axis=-1, keepdims=True)
        xn_ref[s * 128 : (s + 1) * 128, :] = (cen * lax.rsqrt(var + EPS) * gain).astype(BF16)
    wcat = jnp.concatenate([w1_ref[...]] * 4 + [w2_ref[...]] * 4, axis=0)
    for s in range(8):
        both = lax.dot_general(
            xn_ref[s * 128 : (s + 1) * 128, :],
            wcat,
            (((1,), (1,)), ((), ())),
            preferred_element_type=F32,
        )
        tf_ref[pl.ds(s, 128, stride=8), :] = both[:, :128]
        right = both[:, 128:].T
        rx_ref[pl.ds(s, 32, stride=8), :] = right[:32]
    lane = lax.broadcasted_iota(jnp.int32, (8, 128), 1) // 32
    for kk in range(2):
        for hh in range(2):
            for yy in range(2):
                gg = yy * 4 + hh * 2 + kk
                for g in range(4):
                    base = (gg * 16 + g * 4) * 8
                    tile = tf_ref[base : base + 8, :]
                    for e in range(1, 4):
                        other = tf_ref[base + e * 8 : base + e * 8 + 8, :]
                        tile = jnp.where(lane == e, other, tile)
                    lx_ref[kk, hh * 2 + yy, :, g * 128 : (g + 1) * 128] = tile

    pl.semaphore_wait(barrier, 20)

    def swap(n):
        if n == 0:
            src, dst = rx_ref.at[pl.ds(pl.multiple_of((1 - core) * 128, 128), 128)], xr_ref.at[core]
        else:
            src, dst = lx_ref.at[1 - core], xl_ref.at[core]
        return pltpu.make_async_remote_copy(
            src_ref=src,
            dst_ref=dst,
            send_sem=xsend.at[n],
            recv_sem=xrecv.at[n],
            device_id=sib,
            device_id_type=MESH,
        )

    def swap_in(n):
        dst = xr_ref.at[1 - core] if n == 0 else xl_ref.at[1 - core]
        return pltpu.make_async_remote_copy(
            src_ref=dst,
            dst_ref=dst,
            send_sem=xsend.at[n],
            recv_sem=xrecv.at[n],
            device_id=sib,
            device_id_type=MESH,
        )

    swap(1).start()
    swap(0).start()
    xr_ref[core] = rx_ref[pl.ds(pl.multiple_of(core * 128, 128), 128), :]
    xl_ref[core] = lx_ref[core]

    def zmessage(way, d):
        last = 8 - way
        return (last,) if d < last else ()

    def half_of(zz):
        return ((zz + 32) % 16) // 8

    def zparts(way, origin, d):
        sgn = 1 - 2 * way
        part = half_of(origin + sgn * d)
        count = 0
        for e in zmessage(way, d):
            count = count + (half_of(origin + sgn * e) + part) % 2
        return part, count

    def zcopy(way, origin, part, d, hop):
        piece = lz_ref.at[origin] if part is None else lz_ref.at[origin, part]
        return pltpu.make_async_remote_copy(
            src_ref=piece,
            dst_ref=piece,
            send_sem=zsend.at[way, d],
            recv_sem=zrecv.at[origin],
            device_id=zdev(hop),
            device_id_type=MESH,
        )

    def zeither(way, origin, part, count, d, hop, act):
        if not zmessage(way, d):
            act(zcopy(way, origin, part, d, hop))
            return

        @pl.when(count > 0)
        def _():
            act(zcopy(way, origin, None, d, hop))

        @pl.when(count == 0)
        def _():
            act(zcopy(way, origin, part, d, hop))

    zfrom = {d: (d - 1, 1) for d in range(1, 9)}

    def zput(way, d, act):
        at_d, hop = zfrom[d]
        sgn = 1 - 2 * way
        origin = (z - sgn * at_d + 16) % 16
        part, count = zparts(way, origin, d)
        zeither(way, origin, part, count, d, sgn * hop, act)

    def zget(way, d):
        sgn = 1 - 2 * way
        origin = (z - sgn * d + 16) % 16
        part, count = zparts(way, origin, d)
        zeither(way, origin, zh, count, d, 1, lambda copy: copy.wait_recv())
        return origin

    def pcopy(origin, py2):
        cc = origin % 8
        return pltpu.make_async_remote_copy(
            src_ref=lz_ref.at[origin, zh, py2],
            dst_ref=lb_ref.at[(origin // 8) * 16 + x * 4 + y],
            send_sem=psend.at[0],
            recv_sem=precv.at[0],
            device_id=(rows_of(cc // 2, (cc % 2) * 2 + py2, zh, core), zl),
            device_id_type=MESH,
        )

    def spread(origin):
        cc = origin % 8

        def body(py2, _):
            here = jnp.logical_and(cc // 2 == x, (cc % 2) * 2 + py2 == y)

            @pl.when(here)
            def _():
                lb_ref[(origin // 8) * 16 + x * 4 + y] = lz_ref[origin, zh, py2]

            @pl.when(jnp.logical_not(here))
            def _():
                pcopy(origin, py2).start()

            return 0

        lax.fori_loop(0, 2, body, 0)

    def start(copy):
        copy.start()

    def sent(copy):
        copy.wait_send()

    swap_in(1).wait_recv()
    for hy in range(4):
        for g in range(4):
            cols = slice(g * 128, (g + 1) * 128)
            lz_ref[z, hy // 2, hy % 2, :, cols] = jnp.concatenate(
                [xl_ref[0, hy, :, cols], xl_ref[1, hy, :, cols]], axis=0
            ).astype(BF16)
    for way in range(2):
        zput(way, 1, start)

    mine = zh * 16 + x * 4 + y
    swap_in(0).wait_recv()
    for q in range(16):
        rb_ref[core, mine, :, q * 128 : (q + 1) * 128] = jnp.concatenate(
            [xr_ref[0, q * 8 : (q + 1) * 8, :], xr_ref[1, q * 8 : (q + 1) * 8, :]], axis=0
        ).astype(BF16)

    def at(da, db):
        px = (x + da * (1 - core) + db * core + 4) % 4
        py = (y + da * core + db * (1 - core) + 4) % 4
        return px, py

    def slot_of(da, db, hh):
        px, py = at(da, db)
        return hh * 16 + px * 4 + py

    def dev_of(da, db):
        px, py = at(da, db)
        return (rows_of(px, py, zh, core), zl)

    def rblocks(count, sem):
        return pltpu.make_async_remote_copy(
            src_ref=rb_ref.at[core, pl.ds(0, count)],
            dst_ref=rb_ref.at[core, pl.ds(0, count)],
            send_sem=rsend.at[0],
            recv_sem=rrecv.at[sem],
            device_id=sib,
            device_id_type=MESH,
        )

    def rfull(slot, dev, sem):
        return pltpu.make_async_remote_copy(
            src_ref=rb_ref.at[core, slot],
            dst_ref=rb_ref.at[core, slot],
            send_sem=rsend.at[0],
            recv_sem=rrecv.at[sem],
            device_id=dev,
            device_id_type=MESH,
        )

    def rhalf(slot, part, dev, sem):
        piece = rb_ref.at[core, slot, :, pl.ds(part * 1024, 1024)]
        return pltpu.make_async_remote_copy(
            src_ref=piece,
            dst_ref=piece,
            send_sem=rsend.at[0],
            recv_sem=rrecv.at[sem],
            device_id=dev,
            device_id_type=MESH,
        )

    def scopy(slot):
        return pltpu.make_async_remote_copy(
            src_ref=rb_ref.at[core, slot],
            dst_ref=rb_ref.at[core, slot],
            send_sem=sibsend.at[0],
            recv_sem=sibrecv.at[0],
            device_id=sib,
            device_id_type=MESH,
        )

    steps = (0, -1, 1, 2)

    def begin(hh):
        slot = slot_of(0, 0, hh)
        for da, db, sem in ((1, 0, 0), (-1, 0, 1), (0, 1, 3), (0, -1, 4)):
            rfull(slot, dev_of(da, db), sem).start()
        scopy(slot).start()

    def to_b(slot, n):
        rfull(slot, dev_of(0, 1), 3 + 2 * n).start()
        rfull(slot, dev_of(0, -1), 4 + 2 * n).start()
        scopy(slot).start()

    def ring_a(hh):
        for part in range(2):
            step = 1 - 2 * part
            slot = slot_of(-step, 0, hh)
            rblocks(1, part).wait_recv()
            rhalf(slot, part, dev_of(step, 0), 2).start()
            to_b(slot, 1 + part)

    def ring_a_far(hh):
        rblocks(1, 2).wait_recv()
        to_b(slot_of(2, 0, hh), 3)

    def ring_b(hh, n):
        for part in range(2):
            step = 1 - 2 * part
            slot = slot_of(steps[n], -step, hh)
            rblocks(1, 3 + 2 * n + part).wait_recv()
            rhalf(slot, part, dev_of(0, step), 11).start()
            scopy(slot).start()

    def ring_b_far(hh):
        rblocks(4, 11).wait_recv()
        for n in range(4):
            scopy(slot_of(steps[n], 2, hh)).start()

    def begin_straight(hh):
        slot = slot_of(0, 0, hh)
        for step, sem in ((1, 13), (-1, 14), (2, 15)):
            rfull(slot, dev_of(step, 0), sem).start()
        for step in (1, -1, 2):
            rfull(slot, dev_of(0, step), 16).start()
        scopy(slot).start()

    def ring_a_straight(hh):
        for n in range(1, 4):
            slot = slot_of(steps[n], 0, hh)
            rblocks(1, 12 + n).wait_recv()
            for step in (1, -1, 2):
                rfull(slot, dev_of(0, step), 16 + n).start()
            scopy(slot).start()

    def ring_b_straight(hh, n):
        rblocks(3, 16 + n).wait_recv()
        for db in (-1, 1, 2):
            scopy(slot_of(steps[n], db, hh)).start()


    def rout(part):
        return pltpu.make_async_remote_copy(
            src_ref=rb_ref.at[core, mine, :, pl.ds(part * 1024, 1024)],
            dst_ref=ry_ref.at[part],
            send_sem=rysend.at[part],
            recv_sem=ryrecv.at[part],
            device_id=zdev(4 - 8 * part),
            device_id_type=MESH,
        )

    def ron(part):
        slot = half_of(z - 4 + 8 * part) * 16 + x * 4 + y
        return pltpu.make_async_remote_copy(
            src_ref=ry_ref.at[part],
            dst_ref=rb_ref.at[core, slot, :, pl.ds(part * 1024, 1024)],
            send_sem=rysend.at[2 + part],
            recv_sem=rrecv.at[12],
            device_id=zdev(4 - 8 * part),
            device_id_type=MESH,
        )

    rout(0).start()
    rout(1).start()
    begin(zh)
    spread(z)

    loads[4].wait()
    for p in range(32):
        w3f_ref[pl.ds(p, 32, stride=32), :] = w3_ref[p * 32 : (p + 1) * 32, :].astype(F32)
    for n in range(8):
        wt_ref[:, n * 128 : (n + 1) * 128] = w3f_ref[n * 128 : (n + 1) * 128, :].T.astype(BF16)

    def zstep(d):
        ways = range(1 if d == 8 else 2)
        origins = []
        for way in ways:
            origins.append(zget(way, d))
            for nxt, (at_d, _) in zfrom.items():
                if at_d == d and nxt <= 8 - way:
                    zput(way, nxt, start)
        for origin in origins:
            spread(origin)

    other = 1 - zh
    ring_a(zh)
    zstep(1)
    ring_b(zh, 0)
    for part in range(2):
        rout(part).wait_recv()
        ron(part).start()
    ring_a_far(zh)
    zstep(2)
    ring_b(zh, 1)
    ring_b(zh, 2)
    zstep(3)
    rblocks(1, 12).wait_recv()
    begin_straight(other)
    ring_b(zh, 3)
    zstep(4)
    zstep(5)
    ring_a_straight(other)
    ring_b_far(zh)
    zstep(6)
    ring_b_straight(other, 0)
    zstep(7)
    ring_b_straight(other, 1)
    zstep(8)
    ring_b_straight(other, 2)
    ring_b_straight(other, 3)

    pltpu.make_async_remote_copy(
        src_ref=lb_ref.at[pl.ds(0, 30)],
        dst_ref=lb_ref.at[pl.ds(0, 30)],
        send_sem=psend.at[0],
        recv_sem=precv.at[0],
        device_id=sib,
        device_id_type=MESH,
    ).wait_recv()
    for n in range(4):
        for m in range(4):
            lt_ref[m * 128 : (m + 1) * 128, n * 128 : (n + 1) * 128] = (
                lb_ref[n * 8 : (n + 1) * 8, :, m * 128 : (m + 1) * 128].reshape(128, 128).T
            )

    pltpu.make_async_remote_copy(
        src_ref=rb_ref.at[1 - core],
        dst_ref=rb_ref.at[1 - core],
        send_sem=sibsend.at[0],
        recv_sem=sibrecv.at[0],
        device_id=sib,
        device_id_type=MESH,
    ).wait_recv()

    for h in range(2):

        def outer(qb, _, h=h):
            off = pl.multiple_of(qb * 512, 512)
            right = rb_ref[h, :, :, pl.ds(off, 512)].reshape(512, 512)
            prod = jnp.dot(lt_ref[...], right, preferred_element_type=F32).astype(BF16)
            row = pl.multiple_of((h * 16 + qb * 4) * 32, 128)
            for i in range(16):
                for q in range(4):
                    oall_ref[
                        i // 2, pl.ds(row + q * 32, 32), (i % 2) * 128 : (i % 2 + 1) * 128
                    ] = prod[i * 32 : (i + 1) * 32, q * 128 : (q + 1) * 128]
            return 0

        lax.fori_loop(0, 4, outer, 0)

    for load in loads[5:]:
        load.wait()
    gain2 = g2_ref[...]

    def contract(n, _):
        for m in range(4):
            up = jnp.dot(wt_ref[...], oall_ref[n * 4 + m], preferred_element_type=F32)
            for k in range(2):
                i = n * 8 + m * 2 + k
                mid_ref[i] = cpl_ref[i].astype(F32) + up[:, k * 128 : (k + 1) * 128].T * (
                    1.0 / 512.0
                )
        return 0

    lax.fori_loop(0, 2, contract, 0)

    def norm_pair(n, _):
        mid = mid_ref[pl.ds(n * 4, 4)].reshape(512, 128)
        mean = jnp.mean(mid, axis=-1, keepdims=True)
        cen = mid - mean
        var = jnp.mean(cen * cen, axis=-1, keepdims=True)
        nrm_ref[n] = (cen * lax.rsqrt(var + EPS) * gain2).astype(BF16)
        return 0

    lax.fori_loop(0, 4, norm_pair, 0)

    def result(n):
        return pltpu.make_async_copy(
            res_ref.at[pl.ds(n * 4, 4)], out_hbm.at[pl.ds(n * 4, 4)], out_sem.at[n]
        )

    def transition(n, _):
        hidden = jnp.maximum(
            jnp.dot(nrm_ref[n], wa_ref[...], preferred_element_type=F32), 0.0
        ).astype(BF16)
        res = mid_ref[pl.ds(n * 4, 4)].reshape(512, 128) + jnp.dot(
            hidden, wb_ref[...], preferred_element_type=F32
        )
        res_ref[pl.ds(n * 4, 4)] = res.astype(BF16).reshape(4, 128, 128)
        result(n).start()
        return 0

    lax.fori_loop(0, 4, transition, 0)

    swap(0).wait_send()
    swap(1).wait_send()
    for ref, sem in (
        (rb_ref.at[core, pl.ds(0, 30)], rsend),
        (rb_ref.at[core], sibsend),
        (lb_ref.at[pl.ds(0, 30)], psend),
    ):
        pltpu.make_async_remote_copy(
            src_ref=ref,
            dst_ref=ref,
            send_sem=sem.at[0],
            recv_sem=sibrecv.at[0],
            device_id=sib,
            device_id_type=MESH,
        ).wait_send()
    for part in range(2):
        rout(part).wait_send()
        ron(part).wait_send()
    for d in range(1, 9):
        for way in range(1 if d == 8 else 2):
            zput(way, d, sent)
    for n in range(4):
        result(n).wait()


def on_device(x, cpl, g1, w1, w2, w3, g2, wa, wb):
    hbm = pl.BlockSpec(memory_space=pltpu.HBM)
    dma = pltpu.SemaphoreType.DMA
    args = (x, cpl, g1.reshape(1, 256), w1.T, w2.T, w3, g2.reshape(1, 128), wa, wb)
    return pl.pallas_call(
        kernel,
        out_shape=jax.ShapeDtypeStruct(cpl.shape, BF16),
        in_specs=[hbm] * len(args),
        out_specs=hbm,
        scratch_shapes=[pltpu.VMEM(a.shape, a.dtype) for a in args]
        + [
            pltpu.VMEM((1024, 128), F32),
            pltpu.VMEM((128, 1024), BF16),
            pltpu.VMEM((1024, 256), BF16),
            pltpu.VMEM((1024, 128), F32),
            pltpu.VMEM((2, 4, 8, 512), F32),
            pltpu.VMEM((256, 128), F32),
            pltpu.VMEM((2, 4, 8, 512), F32),
            pltpu.VMEM((2, 128, 128), F32),
            pltpu.VMEM((16, 2, 2, 16, 512), BF16),
            pltpu.VMEM((32, 16, 512), BF16),
            pltpu.VMEM((512, 512), BF16),
            pltpu.VMEM((2, 32, 16, 2048), BF16),
            pltpu.VMEM((2, 16, 1024), BF16),
            pltpu.VMEM((8, 1024, 256), BF16),
            pltpu.VMEM((16, 128, 128), F32),
            pltpu.VMEM((4, 512, 128), BF16),
            pltpu.VMEM((16, 128, 128), BF16),
            dma((len(args),)),
            dma((4,)),
            dma((2,)),
            dma((2,)),
            dma((1,)),
            dma((20,)),
            dma((1,)),
            dma((1,)),
            dma((4,)),
            dma((2,)),
            dma((2, 9)),
            dma((16,)),
            dma((1,)),
            dma((1,)),
        ],
        compiler_params=pltpu.CompilerParams(
            collective_id=0, has_side_effects=True, vmem_limit_bytes=66500000
        ),
    )(*args)


def solution(mesh):
    return jax.shard_map(
        on_device,
        mesh=mesh,
        in_specs=(
            P("rows", "cols", None),
            P("rows", "cols", None),
            P(),
            P(),
            P(),
            P(),
            P(),
            P(),
            P(),
        ),
        out_specs=P("rows", "cols", None),
        check_vma=False,
    )
```
